8 devices in a mesh: dp: 2 (over z, y), tp: 4 (over x, core).
Axes of the slice: x: 2, y: 2, z: 1, core: 2. Of those that a mesh axis runs over, the one named last changes fastest.
Arguments:
- resid_in: bfloat16 [512, 4096], P('dp'), parts along dimension 0
- positions: int32 [512], P('dp'), parts along dimension 0
- k_cache: bfloat16 [512, 256, 8, 128], P('dp', None, 'tp'), parts along dimension 0
- v_cache: bfloat16 [512, 256, 8, 128], P('dp', None, 'tp'), parts along dimension 0
- gain_attn: bfloat16 [4096], replicated
- w_query: bfloat16 [4096, 4096], P(None, 'tp')
- w_key: bfloat16 [4096, 1024], P(None, 'tp')
- w_value: bfloat16 [4096, 1024], P(None, 'tp')
- w_out: bfloat16 [4096, 4096], P('tp')
- gain_mlp: bfloat16 [4096], replicated
- w_gate: bfloat16 [4096, 14336], P(None, 'tp')
- w_up: bfloat16 [4096, 14336], P(None, 'tp')
- w_down: bfloat16 [14336, 4096], P('tp')
Outputs:
- output 1: bfloat16 [512, 4096], P('dp'), parts along dimension 0
- output 2: bfloat16 [512, 256, 8, 128], P('dp', None, 'tp'), parts along dimension 0
- output 3: bfloat16 [512, 256, 8, 128], P('dp', None, 'tp'), parts along dimension 0
There are 2 independent parts. The reference program is written for one: setup_inputs(seed, part) draws one part's arguments, and reference() takes and returns one part's arrays. A program takes and returns all parts, laid end to end along the dimension named above; an argument that names none is the same for every part.
All inputs are finite; a program needn't handle non-finite values.
Results may differ from the reference program's by a relative error of at most 0.0103738.
Values sent between devices are 32-bit elements.
A program may use at most 1 GiB of HBM per device.

```python
import math
import jax
import jax.numpy as jnp
from jax import lax

BATCH_PART = 256
CACHE_LEN = 256
MODEL_DIM = 4096
Q_HEADS = 32
KV_HEADS = 8
HEAD_DIM = 128
FFN_DIM = 14336

EPS = 1e-5
ROPE_THETA = 500000.0
ROPE_FACTOR = 8.0
LOW_FACTOR = 1.0
HIGH_FACTOR = 4.0
ORIG_CTX = 8192.0


def setup_inputs(seed: int = 0, part: int = 0) -> dict:
    part_keys = jax.random.split(jax.random.fold_in(jax.random.key(seed), part), 6)
    weight_keys = jax.random.split(jax.random.key(seed + 1), 11)
    log_len = int(math.log2(CACHE_LEN))
    dim_scale = 1.0 / math.sqrt(MODEL_DIM)
    out_scale = 1.0 / math.sqrt(Q_HEADS * HEAD_DIM)
    ffn_scale = 1.0 / math.sqrt(FFN_DIM)
    q_width = Q_HEADS * HEAD_DIM
    kv_width = KV_HEADS * HEAD_DIM
    resid_in = jax.random.normal(part_keys[0], (BATCH_PART, MODEL_DIM), jnp.float32)
    exponent = jax.random.randint(part_keys[1], (BATCH_PART,), 0, log_len + 1, dtype=jnp.int32)
    upper_bound = jnp.left_shift(jnp.ones((BATCH_PART,), jnp.int32), exponent)
    positions = jax.random.randint(part_keys[2], (BATCH_PART,), 0, upper_bound, dtype=jnp.int32)
    positions = positions.at[0].set(CACHE_LEN - 1).at[1].set(0)
    cache_shape = (BATCH_PART, CACHE_LEN, KV_HEADS, HEAD_DIM)
    k_cache = jax.random.normal(part_keys[3], cache_shape, jnp.float32)
    v_mean = 0.7 * jax.random.normal(part_keys[4], (BATCH_PART, 1, KV_HEADS, HEAD_DIM), jnp.float32)
    v_cache = v_mean + jax.random.normal(part_keys[5], cache_shape, jnp.float32)
    gain_attn = 1.0 + 0.3 * jax.random.normal(weight_keys[0], (MODEL_DIM,), jnp.float32)
    w_query = jax.random.normal(weight_keys[1], (MODEL_DIM, q_width), jnp.float32) * dim_scale
    w_key = jax.random.normal(weight_keys[2], (MODEL_DIM, kv_width), jnp.float32) * dim_scale
    w_value = jax.random.normal(weight_keys[3], (MODEL_DIM, kv_width), jnp.float32) * dim_scale
    w_out = jax.random.normal(weight_keys[4], (q_width, MODEL_DIM), jnp.float32) * out_scale
    gain_mlp = 1.0 + 0.3 * jax.random.normal(weight_keys[5], (MODEL_DIM,), jnp.float32)
    w_gate = jax.random.normal(weight_keys[6], (MODEL_DIM, FFN_DIM), jnp.float32) * dim_scale
    w_up = jax.random.normal(weight_keys[7], (MODEL_DIM, FFN_DIM), jnp.float32) * dim_scale
    w_down = jax.random.normal(weight_keys[8], (FFN_DIM, MODEL_DIM), jnp.float32) * ffn_scale
    return dict(resid_in=resid_in.astype(jnp.bfloat16), positions=positions,
                k_cache=k_cache.astype(jnp.bfloat16), v_cache=v_cache.astype(jnp.bfloat16),
                gain_attn=gain_attn.astype(jnp.bfloat16), w_query=w_query.astype(jnp.bfloat16),
                w_key=w_key.astype(jnp.bfloat16), w_value=w_value.astype(jnp.bfloat16),
                w_out=w_out.astype(jnp.bfloat16), gain_mlp=gain_mlp.astype(jnp.bfloat16),
                w_gate=w_gate.astype(jnp.bfloat16), w_up=w_up.astype(jnp.bfloat16),
                w_down=w_down.astype(jnp.bfloat16))


def rms_norm(rows_in, gain):
    rows_f = rows_in.astype(jnp.float32)
    mean_sq = jnp.mean(rows_f * rows_f, axis=-1, keepdims=True)
    return (rows_f * lax.rsqrt(mean_sq + EPS) * gain.astype(jnp.float32)).astype(jnp.bfloat16)


def rope_tables(positions, head_dim):
    half_dim = head_dim // 2
    exponents = jnp.arange(half_dim, dtype=jnp.float32) * (2.0 / head_dim)
    inv_freq = 1.0 / jnp.power(ROPE_THETA, exponents)
    wavelen = (2.0 * math.pi) / inv_freq
    smooth = (ORIG_CTX / wavelen - LOW_FACTOR) / (HIGH_FACTOR - LOW_FACTOR)
    blended = (1.0 - smooth) * inv_freq / ROPE_FACTOR + smooth * inv_freq
    inv_freq = jnp.where(wavelen < ORIG_CTX / HIGH_FACTOR, inv_freq,
                         jnp.where(wavelen > ORIG_CTX / LOW_FACTOR, inv_freq / ROPE_FACTOR, blended))
    angles = positions.astype(jnp.float32)[:, None] * inv_freq[None, :]
    return jnp.cos(angles), jnp.sin(angles)


def apply_rope(vectors, cos_t, sin_t):
    half_dim = vectors.shape[-1] // 2
    lower_half = vectors[..., :half_dim]
    upper_half = vectors[..., half_dim:]
    cos_b = cos_t[:, None, :]
    sin_b = sin_t[:, None, :]
    return jnp.concatenate([lower_half * cos_b - upper_half * sin_b,
                            upper_half * cos_b + lower_half * sin_b], axis=-1)


def reference(resid_in, positions, k_cache, v_cache, gain_attn, w_query, w_key, w_value,
              w_out, gain_mlp, w_gate, w_up, w_down):
    group_size = Q_HEADS // KV_HEADS
    n_seqs = resid_in.shape[0]
    normed = rms_norm(resid_in, gain_attn)
    queries = jnp.dot(normed, w_query, preferred_element_type=jnp.float32).astype(jnp.bfloat16)
    key_new = jnp.dot(normed, w_key, preferred_element_type=jnp.float32).astype(jnp.bfloat16)
    value_new = jnp.dot(normed, w_value, preferred_element_type=jnp.float32).astype(jnp.bfloat16)
    cos_t, sin_t = rope_tables(positions, HEAD_DIM)
    queries = apply_rope(queries.reshape(n_seqs, Q_HEADS, HEAD_DIM).astype(jnp.float32), cos_t, sin_t)
    queries = queries.astype(jnp.bfloat16)
    key_new = apply_rope(key_new.reshape(n_seqs, KV_HEADS, HEAD_DIM).astype(jnp.float32), cos_t, sin_t)
    key_new = key_new.astype(jnp.bfloat16)
    value_new = value_new.reshape(n_seqs, KV_HEADS, HEAD_DIM)
    slot_hit = (jnp.arange(CACHE_LEN)[None, :] == positions[:, None])[:, :, None, None]
    k_full = jnp.where(slot_hit, key_new[:, None], k_cache)
    v_full = jnp.where(slot_hit, value_new[:, None], v_cache)
    scale = 1.0 / math.sqrt(HEAD_DIM)

    def one_seq(seq_items):
        q_seq, k_seq, v_seq, pos_seq = seq_items
        q_grp = q_seq.reshape(KV_HEADS, group_size, HEAD_DIM).astype(jnp.float32)
        scores = jnp.einsum('kgd,skd->kgs', q_grp, k_seq.astype(jnp.float32)) * scale
        valid = jnp.arange(CACHE_LEN) <= pos_seq
        scores = jnp.where(valid[None, None, :], scores, -jnp.inf)
        attn_prob = jax.nn.softmax(scores, axis=-1).astype(jnp.bfloat16)
        attn_seq = jnp.einsum('kgs,skd->kgd', attn_prob.astype(jnp.float32), v_seq.astype(jnp.float32))
        return attn_seq.astype(jnp.bfloat16).reshape(Q_HEADS * HEAD_DIM)

    attn_out = lax.map(one_seq, (queries, k_full, v_full, positions))
    y_full = jnp.dot(attn_out, w_out, preferred_element_type=jnp.float32)
    resid_mid = (resid_in.astype(jnp.float32) + y_full).astype(jnp.bfloat16)
    normed_mlp = rms_norm(resid_mid, gain_mlp)
    gate_proj = jnp.dot(normed_mlp, w_gate, preferred_element_type=jnp.float32).astype(jnp.bfloat16)
    up_proj = jnp.dot(normed_mlp, w_up, preferred_element_type=jnp.float32).astype(jnp.bfloat16)
    hidden = (jax.nn.silu(gate_proj.astype(jnp.float32)) * up_proj.astype(jnp.float32)).astype(jnp.bfloat16)
    z_full = jnp.dot(hidden, w_down, preferred_element_type=jnp.float32)
    resid_out = (resid_mid.astype(jnp.float32) + z_full).astype(jnp.bfloat16)
    return resid_out, k_full, v_full
```

```python
import functools
import math
import jax
import jax.numpy as jnp
from jax import lax
from jax.experimental import pallas as pl
from jax.experimental.pallas import tpu as pltpu
from jax.sharding import PartitionSpec as P

EPS = 1e-5
ROPE_THETA = 500000.0
ROPE_FACTOR = 8.0
LOW_FACTOR = 1.0
HIGH_FACTOR = 4.0
ORIG_CTX = 8192.0

F32 = jnp.float32
BF16 = jnp.bfloat16
SEQS = 256
SLOTS = 256
WIDTH = 4096
HALF = WIDTH // 2
HD = 128
QH = 8
KVH = 2
FFN = 3584
VMEM_ALL = 67043328

ROWS = 32
CHUNKS = SEQS // ROWS
BLK = 8
BLKS = ROWS // BLK
KVSLOTS = 3
TN = 512
NT = HALF // TN
WSLOTS = 5
GT = FFN // TN
N_TILES = 2 * GT + 2 * NT


def rope_tables(positions, head_dim):
    half_dim = head_dim // 2
    exponents = jnp.arange(half_dim, dtype=jnp.float32) * (2.0 / head_dim)
    inv_freq = 1.0 / jnp.power(ROPE_THETA, exponents)
    wavelen = (2.0 * math.pi) / inv_freq
    smooth = (ORIG_CTX / wavelen - LOW_FACTOR) / (HIGH_FACTOR - LOW_FACTOR)
    blended = (1.0 - smooth) * inv_freq / ROPE_FACTOR + smooth * inv_freq
    inv_freq = jnp.where(wavelen < ORIG_CTX / HIGH_FACTOR, inv_freq,
                         jnp.where(wavelen > ORIG_CTX / LOW_FACTOR, inv_freq / ROPE_FACTOR, blended))
    angles = positions.astype(jnp.float32)[:, None] * inv_freq[None, :]
    return jnp.cos(angles), jnp.sin(angles)


def norm_rows(rows_f, gain_f):
    mean_sq = jnp.mean(rows_f * rows_f, axis=-1, keepdims=True)
    return (rows_f * lax.rsqrt(mean_sq + EPS) * gain_f).astype(BF16)


def qkv_kernel(gain_ref, cos_ref, sin_ref, x_hbm, wq_hbm, wk_hbm, wv_hbm,
               q_ref, kx_ref, vx_ref, kn_ref, vn_ref, x_ref, h_ref, w_ref, x_sem, w_sem):
    cols = 256
    nq = QH * HD // cols
    load_x = pltpu.make_async_copy(x_hbm, x_ref, x_sem)
    load_x.start()
    loads = [pltpu.make_async_copy(wq_hbm.at[:, i * cols:(i + 1) * cols], w_ref.at[i], w_sem.at[i])
             for i in range(nq)]
    loads.append(pltpu.make_async_copy(wk_hbm, w_ref.at[nq], w_sem.at[nq]))
    loads.append(pltpu.make_async_copy(wv_hbm, w_ref.at[nq + 1], w_sem.at[nq + 1]))
    for load in loads:
        load.start()
    load_x.wait()
    gain_f = gain_ref[...].astype(F32)

    def norm_step(i, _):
        rows = pl.ds(pl.multiple_of(i * 16, 16), 16)
        h_ref[rows, :] = norm_rows(x_ref[rows, :].astype(F32), gain_f)
        return 0

    lax.fori_loop(0, SEQS // 16, norm_step, 0)

    def rotate(v):
        return (v * cos_ref[...] + pltpu.roll(v, HD // 2, 1) * sin_ref[...]).astype(BF16).astype(F32)

    for i, load in enumerate(loads):
        load.wait()
        prod = jnp.dot(h_ref[...], w_ref[i], preferred_element_type=F32).astype(BF16).astype(F32)
        for j in range(2):
            head = prod[:, j * HD:(j + 1) * HD]
            if i < nq:
                q_ref[:, 2 * i + j, :] = rotate(head)
            elif i == nq:
                head = rotate(head)
                kn_ref[:, j * HD:(j + 1) * HD] = head.astype(BF16)
                for g in range(QH // KVH):
                    kx_ref[:, j * (QH // KVH) + g, :] = head
            else:
                vn_ref[:, j * HD:(j + 1) * HD] = head.astype(BF16)
                for g in range(QH // KVH):
                    vx_ref[:, j * (QH // KVH) + g, :] = head


def qkv(resid_in, gain, cos_t, sin_t, w_query, w_key, w_value):
    vmem = pl.BlockSpec(memory_space=pltpu.VMEM)
    hbm = pl.BlockSpec(memory_space=pl.ANY)
    shape = jax.ShapeDtypeStruct
    return pl.pallas_call(
        qkv_kernel,
        name="qkv",
        out_shape=(shape((SEQS, QH, HD), F32), shape((SEQS, QH, HD), F32), shape((SEQS, QH, HD), F32),
                   shape((SEQS, KVH * HD), BF16), shape((SEQS, KVH * HD), BF16)),
        in_specs=[vmem] * 3 + [hbm] * 4,
        out_specs=(vmem,) * 5,
        scratch_shapes=[pltpu.VMEM((SEQS, WIDTH), BF16), pltpu.VMEM((SEQS, WIDTH), BF16),
                        pltpu.VMEM((6, WIDTH, 256), BF16), pltpu.SemaphoreType.DMA, pltpu.SemaphoreType.DMA((6,))],
        compiler_params=pltpu.CompilerParams(vmem_limit_bytes=VMEM_ALL),
        cost_estimate=pl.CostEstimate(flops=2 * SEQS * WIDTH * 1536, bytes_accessed=16 * 2**20, transcendentals=0),
    )(gain, cos_t, sin_t, resid_in, w_query, w_key, w_value)


CBLK = 16
CSLOTS = 12


def cache_kernel(pos_ref, kn_ref, vn_ref, k_hbm, v_hbm, after_hbm, k_out, v_out, buf, in_sem, out_sem):
    steps = [(src, dst, new, i) for i in range(SEQS // CBLK)
             for src, dst, new in ((k_hbm, k_out, kn_ref), (v_hbm, v_out, vn_ref))]
    n = len(steps)
    ahead = CSLOTS // 2

    def load(s):
        src, _, _, i = steps[s]
        return pltpu.make_async_copy(src.at[pl.ds(i * CBLK, CBLK)], buf.at[s % CSLOTS], in_sem.at[s % CSLOTS])

    def save(s):
        _, dst, _, i = steps[s]
        return pltpu.make_async_copy(buf.at[s % CSLOTS], dst.at[pl.ds(i * CBLK, CBLK)], out_sem.at[s % CSLOTS])

    for s in range(ahead):
        load(s).start()
    for s in range(n):
        if s + ahead < n:
            if s + ahead >= CSLOTS:
                save(s + ahead - CSLOTS).wait()
            load(s + ahead).start()
        load(s).wait()
        _, _, new, i = steps[s]

        def patch(j, _, new=new, i=i, s=s):
            row = i * CBLK + j
            buf[s % CSLOTS, j, pos_ref[row]] = new[row]
            return 0

        lax.fori_loop(0, CBLK, patch, 0)
        save(s).start()
    for s in range(n - CSLOTS, n):
        save(s).wait()


def write_caches(positions, kn, vn, k_cache, v_cache, after):
    vmem = pl.BlockSpec(memory_space=pltpu.VMEM)
    hbm = pl.BlockSpec(memory_space=pl.ANY)
    cache = jax.ShapeDtypeStruct(k_cache.shape, BF16)
    return pl.pallas_call(
        cache_kernel,
        name="write_caches",
        out_shape=(cache, cache),
        in_specs=[pl.BlockSpec(memory_space=pltpu.SMEM), vmem, vmem, hbm, hbm, hbm],
        out_specs=(hbm, hbm),
        scratch_shapes=[pltpu.VMEM((CSLOTS, CBLK, SLOTS, KVH, HD), BF16),
                        pltpu.SemaphoreType.DMA((CSLOTS,)), pltpu.SemaphoreType.DMA((CSLOTS,))],
        compiler_params=pltpu.CompilerParams(vmem_limit_bytes=56 * 2**20),
        cost_estimate=pl.CostEstimate(flops=2 * 10**10, bytes_accessed=128 * 2**20, transcendentals=0),
    )(positions, kn, vn, k_cache, v_cache, after)


def layer_kernel(pos_ref, q_ref, kx_ref, vx_ref, res_ref, gain_ref, k_hbm, v_hbm, wo_hbm, wg_hbm, wu_hbm, wd_hbm,
                 x1_ref, z_ref, kbuf, vbuf, wo, o3, o2, ybuf, rb1, sb, rb2, tb, h2, act, gbuf, wbuf,
                 k_sem, v_sem, wo_sem, w_sem, s1, r1, s2, r2, s3, r3, s4, r4):
    tp = lax.axis_index("tp")
    mine = lax.rem(tp, 2)
    other = 1 - mine
    partner = tp + 1 - 2 * mine
    peer = lax.rem(tp + 2, 4)

    def load_kv(g):
        slot = lax.rem(g, KVSLOTS)
        seqs = pl.ds(g * BLK, BLK)
        return (pltpu.make_async_copy(k_hbm.at[seqs], kbuf.at[slot], k_sem.at[slot]),
                pltpu.make_async_copy(v_hbm.at[seqs], vbuf.at[slot], v_sem.at[slot]))

    for g in range(KVSLOTS):
        for copy in load_kv(g):
            copy.start()

    barrier = pltpu.get_barrier_semaphore()
    for device in (partner, peer):
        pl.semaphore_signal(barrier, inc=1, device_id={"tp": device}, device_id_type=pl.DeviceIdType.MESH)
    pl.semaphore_wait(barrier, 2)

    load_wo = [pltpu.make_async_copy(wo_hbm.at[:, pl.ds(i * HALF, HALF)], wo.at[i], wo_sem.at[i]) for i in range(2)]
    for copy in load_wo:
        copy.start()

    def remote(src, dst, send, recv, device):
        return pltpu.make_async_remote_copy(src_ref=src, dst_ref=dst, send_sem=send, recv_sem=recv,
                                            device_id={"tp": device}, device_id_type=pl.DeviceIdType.MESH)

    def rows_of(c):
        return pl.ds(pl.multiple_of(c * ROWS, ROWS), ROWS)

    def send1(c):
        return remote(ybuf.at[other, :, rows_of(c)], rb1.at[:, rows_of(c)], s1.at[c], r1.at[c], partner)

    def send2(c):
        return remote(sb.at[:, rows_of(c)], rb2.at[:, rows_of(c)], s2.at[c], r2.at[c], peer)

    def send3(c):
        return remote(tb.at[mine, :, rows_of(c)], tb.at[mine, :, rows_of(c)], s3.at[c], r3.at[c], partner)

    def recv3(c):
        return remote(tb.at[other, :, rows_of(c)], tb.at[other, :, rows_of(c)], s3.at[c], r3.at[c], partner)

    def load_gate(t, slot):
        cols = pl.ds(pl.multiple_of(t * TN, TN), TN)
        return pltpu.make_async_copy(wg_hbm.at[:, cols], wbuf.at[slot], w_sem.at[slot])

    def load_up(t, slot):
        cols = pl.ds(pl.multiple_of(t * TN, TN), TN)
        return pltpu.make_async_copy(wu_hbm.at[:, cols], wbuf.at[slot], w_sem.at[slot])

    def load_down(t, slot):
        far = (t < NT).astype(jnp.int32)
        half = far * other + (1 - far) * mine
        start = half * HALF + (t - (1 - far) * NT) * TN
        cols = pl.ds(pl.multiple_of(start, TN), TN)
        return pltpu.make_async_copy(wd_hbm.at[:, cols], wbuf.at[slot, pl.ds(0, FFN)], w_sem.at[slot])

    def start_tile(i):
        slot = lax.rem(i, WSLOTS)
        odd = lax.rem(i, 2)

        @pl.when((i < 2 * GT) & (odd == 0))
        def _():
            load_gate(i // 2, slot).start()

        @pl.when((i < 2 * GT) & (odd == 1))
        def _():
            load_up(i // 2, slot).start()

        @pl.when((i >= 2 * GT) & (i < N_TILES))
        def _():
            load_down(i - 2 * GT, slot).start()

    col = lax.broadcasted_iota(jnp.int32, (QH, KVH * SLOTS), 1)
    row_head = lax.broadcasted_iota(jnp.int32, (QH, KVH * SLOTS), 0) // (QH // KVH)
    col_slot = jnp.where(lax.rem(col, KVH) == row_head, col // KVH, SLOTS)
    scale = 1.0 / math.sqrt(HD)

    def attend(g, base):
        slot = lax.rem(g, KVSLOTS)
        for copy in load_kv(g):
            copy.wait()
        qs = [q_ref[g * BLK + i] for i in range(BLK)]
        score = [lax.dot_general(qs[i].astype(BF16), kbuf[slot, i], (((1,), (1,)), ((), ())),
                                 preferred_element_type=F32) for i in range(BLK)]
        new = [jnp.sum(qs[i] * kx_ref[g * BLK + i].astype(F32), axis=1, keepdims=True) * scale for i in range(BLK)]
        score = [jnp.where(col_slot < pos_ref[g * BLK + i], score[i] * scale, -jnp.inf) for i in range(BLK)]
        top = [jnp.maximum(jnp.max(score[i], axis=1, keepdims=True), new[i]) for i in range(BLK)]
        e = [jnp.exp(score[i] - top[i]) for i in range(BLK)]
        e_new = [jnp.exp(new[i] - top[i]) for i in range(BLK)]
        inv = [1.0 / (jnp.sum(e[i], axis=1, keepdims=True) + e_new[i]) for i in range(BLK)]
        for i in range(BLK):
            prob = (e[i] * inv[i]).astype(BF16)
            prob_new = (e_new[i] * inv[i]).astype(BF16).astype(F32)
            out = jnp.dot(prob, vbuf[slot, i], preferred_element_type=F32)
            out = out + prob_new * vx_ref[g * BLK + i].astype(F32)
            o3[base + i] = out.astype(BF16).astype(F32)

        @pl.when(g + KVSLOTS < SEQS // BLK)
        def _():
            for copy in load_kv(g + KVSLOTS):
                copy.start()

    def project(c, half):
        for n in range(NT):
            ybuf[half, n, rows_of(c), :] = jnp.dot(o2[...], wo[half, :, n * TN:(n + 1) * TN],
                                                   preferred_element_type=F32)

    def stage2(c):
        send1(c).wait_recv()
        sb[:, rows_of(c)] = ybuf[mine, :, rows_of(c)] + rb1[:, rows_of(c)]
        send2(c).start()

    def stage3(c):
        send2(c).wait_recv()
        tb[mine, :, rows_of(c)] = sb[:, rows_of(c)] + rb2[:, rows_of(c)]
        send3(c).start()

    def stage4(c):
        recv3(c).wait_recv()
        gain_f = gain_ref[...].astype(F32)

        def body(i, _):
            rows = pl.ds(pl.multiple_of(c * ROWS + i * 16, 16), 16)
            total = jnp.zeros((16, 1), F32)
            for half in range(2):
                for n in range(NT):
                    cols = slice(half * HALF + n * TN, half * HALF + (n + 1) * TN)
                    x1 = (res_ref[rows, cols].astype(F32) + tb[half, n, rows, :]).astype(BF16)
                    x1_ref[rows, cols] = x1
                    x1_f = x1.astype(F32)
                    total = total + jnp.sum(x1_f * x1_f, axis=1, keepdims=True)
            inv = lax.rsqrt(total * (1.0 / WIDTH) + EPS)
            for n in range(2 * NT):
                cols = slice(n * TN, (n + 1) * TN)
                h2[rows, cols] = (x1_ref[rows, cols].astype(F32) * inv * gain_f[:, cols]).astype(BF16)
            return 0

        lax.fori_loop(0, ROWS // 16, body, 0)

    def chunk(c, _):
        def block(j, _):
            attend(c * BLKS + j, j * BLK)

            @pl.when((j == 0) & (c >= 1))
            def _():
                stage2(c - 1)

            return 0

        lax.fori_loop(0, BLKS, block, 0)
        for j in range(QH):
            o2[:, j * HD:(j + 1) * HD] = o3[:, j, :].astype(BF16)

        @pl.when(c == 0)
        def _():
            for copy in load_wo:
                copy.wait()

        project(c, other)
        send1(c).start()
        project(c, mine)

        @pl.when(c >= CHUNKS - WSLOTS)
        def _():
            start_tile(c - (CHUNKS - WSLOTS))

        @pl.when(c >= 3)
        def _():
            stage3(c - 3)

        @pl.when(c >= 4)
        def _():
            stage4(c - 4)

        return 0

    lax.fori_loop(0, CHUNKS, chunk, 0)
    stage2(CHUNKS - 1)
    stage4(CHUNKS - 4)

    def tail(c, _):
        stage3(c)
        return 0

    def tail4(c, _):
        stage4(c)
        return 0

    lax.fori_loop(CHUNKS - 3, CHUNKS, tail, 0)
    lax.fori_loop(CHUNKS - 3, CHUNKS, tail4, 0)

    def sent(c, _):
        send1(c).wait_send()
        send2(c).wait_send()
        send3(c).wait_send()
        return 0

    lax.fori_loop(0, CHUNKS, sent, 0)

    def mm(lhs_ref, slot, depth, n):
        return jnp.dot(lhs_ref[...], wbuf[slot, 0:depth, n * 256:(n + 1) * 256], preferred_element_type=F32)

    def gate_up(t, _):
        slot = lax.rem(2 * t, WSLOTS)
        load_gate(t, slot).wait()
        for n in range(TN // 256):
            gbuf[:, n * 256:(n + 1) * 256] = mm(h2, slot, WIDTH, n).astype(BF16)
        start_tile(2 * t + WSLOTS)
        slot = lax.rem(2 * t + 1, WSLOTS)
        load_up(t, slot).wait()
        for n in range(TN // 256):
            up = mm(h2, slot, WIDTH, n).astype(BF16).astype(F32)
            gate = gbuf[:, n * 256:(n + 1) * 256].astype(F32)
            act[:, pl.ds(pl.multiple_of(t * TN + n * 256, 256), 256)] = (jax.nn.silu(gate) * up).astype(BF16)
        start_tile(2 * t + 1 + WSLOTS)
        return 0

    lax.fori_loop(0, GT, gate_up, 0)

    def send4(t):
        return remote(ybuf.at[other, t], rb1.at[t], s4.at[t], r4.at[t], partner)

    def down_far(t, _):
        i = 2 * GT + t
        slot = lax.rem(i, WSLOTS)
        load_down(t, slot).wait()
        for n in range(TN // 256):
            ybuf[other, t, :, n * 256:(n + 1) * 256] = mm(act, slot, FFN, n)
        send4(t).start()
        start_tile(i + WSLOTS)
        return 0

    lax.fori_loop(0, NT, down_far, 0)

    def down_near(t, _):
        i = 2 * GT + NT + t
        slot = lax.rem(i, WSLOTS)
        load_down(NT + t, slot).wait()
        send4(t).wait_recv()
        for n in range(TN // 256):
            z_ref[t, :, n * 256:(n + 1) * 256] = mm(act, slot, FFN, n) + rb1[t, :, n * 256:(n + 1) * 256]
        start_tile(i + WSLOTS)
        return 0

    lax.fori_loop(0, NT, down_near, 0)

    def sent4(t, _):
        send4(t).wait_send()
        return 0

    lax.fori_loop(0, NT, sent4, 0)


def layer(positions, q, kx, vx, resid_in, gain, k_rows, v_rows, w_out, w_gate, w_up, w_down):
    vmem = pl.BlockSpec(memory_space=pltpu.VMEM)
    hbm = pl.BlockSpec(memory_space=pl.ANY)
    dma = pltpu.SemaphoreType.DMA
    return pl.pallas_call(
        layer_kernel,
        name="layer",
        out_shape=(jax.ShapeDtypeStruct((SEQS, WIDTH), BF16), jax.ShapeDtypeStruct((NT, SEQS, TN), F32)),
        in_specs=[pl.BlockSpec(memory_space=pltpu.SMEM)] + [vmem] * 5 + [hbm] * 6,
        out_specs=(vmem, vmem),
        scratch_shapes=[
            pltpu.VMEM((KVSLOTS, BLK, KVH * SLOTS, HD), BF16), pltpu.VMEM((KVSLOTS, BLK, KVH * SLOTS, HD), BF16),
            pltpu.VMEM((2, QH * HD, HALF), BF16),
            pltpu.VMEM((ROWS, QH, HD), F32), pltpu.VMEM((ROWS, QH * HD), BF16),
            pltpu.VMEM((2, NT, SEQS, TN), F32), pltpu.VMEM((NT, SEQS, TN), F32), pltpu.VMEM((NT, SEQS, TN), F32),
            pltpu.VMEM((NT, SEQS, TN), F32), pltpu.VMEM((2, NT, SEQS, TN), F32),
            pltpu.VMEM((SEQS, WIDTH), BF16), pltpu.VMEM((SEQS, FFN), BF16), pltpu.VMEM((SEQS, TN), BF16),
            pltpu.VMEM((WSLOTS, WIDTH, TN), BF16),
            dma((KVSLOTS,)), dma((KVSLOTS,)), dma((2,)), dma((WSLOTS,)),
            dma((CHUNKS,)), dma((CHUNKS,)), dma((CHUNKS,)), dma((CHUNKS,)), dma((CHUNKS,)), dma((CHUNKS,)),
            dma((NT,)), dma((NT,))],
        compiler_params=pltpu.CompilerParams(collective_id=0, has_side_effects=True, vmem_limit_bytes=VMEM_ALL),
        cost_estimate=pl.CostEstimate(flops=3 * 10**10, bytes_accessed=180 * 2**20, transcendentals=0),
    )(positions, q, kx, vx, resid_in, gain, k_rows, v_rows, w_out, w_gate, w_up, w_down)


def final_kernel(z_ref, zr_ref, x1_ref, out_ref, tb, send_sem, recv_sem):
    tp = lax.axis_index("tp")
    mine = lax.rem(tp, 2)
    other = 1 - mine
    partner = tp + 1 - 2 * mine
    barrier = pltpu.get_barrier_semaphore()
    pl.semaphore_signal(barrier, inc=1, device_id={"tp": partner}, device_id_type=pl.DeviceIdType.MESH)
    pl.semaphore_wait(barrier, 1)

    def copy(half, t):
        return pltpu.make_async_remote_copy(src_ref=tb.at[half, t], dst_ref=tb.at[half, t], send_sem=send_sem.at[t],
                                            recv_sem=recv_sem.at[t], device_id={"tp": partner},
                                            device_id_type=pl.DeviceIdType.MESH)

    def add(half, t):
        cols = pl.ds(pl.multiple_of(half * HALF + t * TN, TN), TN)
        out_ref[:, cols] = (x1_ref[:, cols].astype(F32) + tb[half, t]).astype(BF16)

    for t in range(NT):
        tb[mine, t] = z_ref[t] + zr_ref[t]
        copy(mine, t).start()
    for t in range(NT):
        add(mine, t)
    for t in range(NT):
        copy(other, t).wait_recv()
        add(other, t)
    for t in range(NT):
        copy(mine, t).wait_send()


def finish(z, z_peer, x1):
    vmem = pl.BlockSpec(memory_space=pltpu.VMEM)
    return pl.pallas_call(
        final_kernel,
        name="finish",
        out_shape=jax.ShapeDtypeStruct((SEQS, WIDTH), BF16),
        in_specs=[vmem] * 3,
        out_specs=vmem,
        scratch_shapes=[pltpu.VMEM((2, NT, SEQS, TN), F32), pltpu.SemaphoreType.DMA((NT,)),
                        pltpu.SemaphoreType.DMA((NT,))],
        compiler_params=pltpu.CompilerParams(collective_id=1, has_side_effects=True, vmem_limit_bytes=24 * 2**20),
        cost_estimate=pl.CostEstimate(flops=2 * 10**8, bytes_accessed=10 * 2**20, transcendentals=0),
    )(z, z_peer, x1)


def solution(mesh):
    def layer_local(resid_in, positions, k_cache, v_cache, gain_attn, w_query, w_key, w_value,
                    w_out, gain_mlp, w_gate, w_up, w_down):
        cos_t, sin_t = rope_tables(positions, HD)
        cos_t = jnp.concatenate([cos_t, cos_t], axis=1)
        sin_t = jnp.concatenate([-sin_t, sin_t], axis=1)
        q, kx, vx, kn, vn = qkv(resid_in, gain_attn.reshape(1, WIDTH), cos_t, sin_t, w_query, w_key, w_value)
        k_rows = k_cache.reshape(SEQS, SLOTS * KVH, HD)
        v_rows = v_cache.reshape(SEQS, SLOTS * KVH, HD)
        x1, z = layer(positions, q, kx, vx, resid_in, gain_mlp.reshape(1, WIDTH), k_rows, v_rows,
                      w_out, w_gate, w_up, w_down)
        z_peer = lax.ppermute(z, 'tp', [(0, 2), (1, 3), (2, 0), (3, 1)])
        k_full, v_full = write_caches(positions, kn.reshape(SEQS, KVH, HD), vn.reshape(SEQS, KVH, HD),
                                      k_cache, v_cache, z)
        resid_out = finish(z, z_peer, x1)
        return resid_out, k_full, v_full

    row_spec = P('dp', None)
    cache_spec = P('dp', None, 'tp', None)
    col_spec = P(None, 'tp')
    split_rows = P('tp', None)
    return jax.shard_map(layer_local, mesh=mesh,
                         in_specs=(row_spec, P('dp'), cache_spec, cache_spec, P(), col_spec, col_spec,
                                   col_spec, split_rows, P(), col_spec, col_spec, split_rows),
                         out_specs=(row_spec, cache_spec, cache_spec), check_vma=False)
```

```python
import functools
import math
import jax
import jax.numpy as jnp
from jax import lax
from jax.experimental import pallas as pl
from jax.experimental.pallas import tpu as pltpu
from jax.sharding import PartitionSpec as P

EPS = 1e-5
ROPE_THETA = 500000.0
ROPE_FACTOR = 8.0
LOW_FACTOR = 1.0
HIGH_FACTOR = 4.0
ORIG_CTX = 8192.0

F32 = jnp.float32
BF16 = jnp.bfloat16
SEQS = 256
SLOTS = 256
WIDTH = 4096
HALF = WIDTH // 2
HD = 128
QH = 8
KVH = 2
FFN = 3584
VMEM_ALL = 67043328

ROWS = 32
CHUNKS = SEQS // ROWS
BLK = 8
BLKS = ROWS // BLK
KVSLOTS = 3
TN = 512
NT = HALF // TN
WSLOTS = 8
GT = FFN // TN
N_TILES = 2 * GT + 2 * NT


def rope_tables(positions, head_dim):
    half_dim = head_dim // 2
    lane = jnp.arange(head_dim)
    exponents = (lane % half_dim).astype(jnp.float32) * (2.0 / head_dim)
    inv_freq = 1.0 / jnp.power(ROPE_THETA, exponents)
    wavelen = (2.0 * math.pi) / inv_freq
    smooth = (ORIG_CTX / wavelen - LOW_FACTOR) / (HIGH_FACTOR - LOW_FACTOR)
    blended = (1.0 - smooth) * inv_freq / ROPE_FACTOR + smooth * inv_freq
    inv_freq = jnp.where(wavelen < ORIG_CTX / HIGH_FACTOR, inv_freq,
                         jnp.where(wavelen > ORIG_CTX / LOW_FACTOR, inv_freq / ROPE_FACTOR, blended))
    angles = positions[:, None].astype(jnp.float32) * inv_freq[None, :]
    sign = jnp.where(lane < half_dim, -1.0, 1.0).astype(jnp.float32)
    return jnp.cos(angles), jnp.sin(angles) * sign[None, :]


CBLK = 8
CSLOTS = 24


def cache_kernel(pos_ref, kn_ref, vn_ref, k_hbm, v_hbm, after_hbm, k_out, v_out, buf, in_sem, out_sem):
    steps = [(src, dst, new, i) for i in range(SEQS // CBLK)
             for src, dst, new in ((k_hbm, k_out, kn_ref), (v_hbm, v_out, vn_ref))]
    n = len(steps)
    ahead = CSLOTS // 2

    def load(s):
        src, _, _, i = steps[s]
        return pltpu.make_async_copy(src.at[pl.ds(i * CBLK, CBLK)], buf.at[s % CSLOTS], in_sem.at[s % CSLOTS])

    def save(s):
        _, dst, _, i = steps[s]
        return pltpu.make_async_copy(buf.at[s % CSLOTS], dst.at[pl.ds(i * CBLK, CBLK)], out_sem.at[s % CSLOTS])

    for s in range(ahead):
        load(s).start()
    for s in range(n):
        if s + ahead < n:
            if s + ahead >= CSLOTS:
                save(s + ahead - CSLOTS).wait()
            load(s + ahead).start()
        load(s).wait()
        _, _, new, i = steps[s]

        def patch(j, _, new=new, i=i, s=s):
            row = i * CBLK + j
            buf[s % CSLOTS, j, pos_ref[row]] = new[row].astype(BF16)
            return 0

        lax.fori_loop(0, CBLK, patch, 0)
        save(s).start()
    for s in range(n - CSLOTS, n):
        save(s).wait()


def write_caches(positions, kn, vn, k_cache, v_cache, after):
    vmem = pl.BlockSpec(memory_space=pltpu.VMEM)
    hbm = pl.BlockSpec(memory_space=pl.ANY)
    cache = jax.ShapeDtypeStruct(k_cache.shape, BF16)
    return pl.pallas_call(
        cache_kernel,
        name="write_caches",
        out_shape=(cache, cache),
        in_specs=[pl.BlockSpec(memory_space=pltpu.SMEM), vmem, vmem, hbm, hbm, hbm],
        out_specs=(hbm, hbm),
        scratch_shapes=[pltpu.VMEM((CSLOTS, CBLK, SLOTS, KVH, HD), BF16),
                        pltpu.SemaphoreType.DMA((CSLOTS,)), pltpu.SemaphoreType.DMA((CSLOTS,))],
        compiler_params=pltpu.CompilerParams(vmem_limit_bytes=56 * 2**20),
        cost_estimate=pl.CostEstimate(flops=2 * 10**10, bytes_accessed=128 * 2**20, transcendentals=0),
    )(positions, kn, vn, k_cache, v_cache, after)


KS = 512
SLABS = WIDTH // KS
QKV = (QH + 2 * KVH) * HD


def spread_gain(gain_ref, gain_row):
    for n in range(WIDTH // 128):
        gain_row[:, n * 128:(n + 1) * 128] = jnp.broadcast_to(gain_ref[n:n + 1, :].astype(F32), (8, 128))


def attention_kernel(pos_ref, cos_ref, sin_ref, gain1_ref, gain2_ref, x_hbm, wq_hbm, wk_hbm, wv_hbm, k_hbm, v_hbm,
                     wo_hbm, x1_ref, h2, kn_ref, vn_ref, x_ref, h_ref, w_ref, acc, q_ref, kx_ref, vx_ref, gain_row,
                     kbuf, vbuf, wo, o3, o2, ybuf, rb1, sb, rb2, tb,
                     x_sem, q_sem, k_sem, v_sem, kc_sem, vc_sem, wo_sem, s1, r1, s2, r2, s3, r3):
    tp = lax.axis_index("tp")
    mine = lax.rem(tp, 2)
    other = 1 - mine
    partner = tp + 1 - 2 * mine
    peer = lax.rem(tp + 2, 4)

    load_x = pltpu.make_async_copy(x_hbm, x_ref, x_sem)
    load_x.start()

    def load_w(i):
        rows = pl.ds(i * KS, KS)
        nq = QH * HD
        return (pltpu.make_async_copy(wq_hbm.at[rows], w_ref.at[rows, pl.ds(0, nq)], q_sem.at[i]),
                pltpu.make_async_copy(wk_hbm.at[rows], w_ref.at[rows, pl.ds(nq, KVH * HD)], k_sem.at[i]),
                pltpu.make_async_copy(wv_hbm.at[rows], w_ref.at[rows, pl.ds(nq + KVH * HD, KVH * HD)], v_sem.at[i]))

    for i in range(SLABS):
        for copy in load_w(i):
            copy.start()

    def load_kv(g):
        slot = lax.rem(g, KVSLOTS)
        seqs = pl.ds(g * BLK, BLK)
        return (pltpu.make_async_copy(k_hbm.at[seqs], kbuf.at[slot], kc_sem.at[slot]),
                pltpu.make_async_copy(v_hbm.at[seqs], vbuf.at[slot], vc_sem.at[slot]))

    for g in range(2):
        for copy in load_kv(g):
            copy.start()
    load_wo = [pltpu.make_async_copy(wo_hbm.at[:, pl.ds(i * HALF, HALF)], wo.at[i], wo_sem.at[i]) for i in range(2)]
    for copy in load_wo:
        copy.start()
    for g in range(2, KVSLOTS):
        for copy in load_kv(g):
            copy.start()

    barrier = pltpu.get_barrier_semaphore()
    for device in (partner, peer):
        pl.semaphore_signal(barrier, inc=1, device_id={"tp": device}, device_id_type=pl.DeviceIdType.MESH)

    spread_gain(gain1_ref, gain_row)
    acc[...] = jnp.zeros_like(acc)
    load_x.wait()

    def norm_step(i, _):
        rows = pl.ds(pl.multiple_of(i * 16, 16), 16)
        total = jnp.zeros((16, 1), F32)
        for n in range(2 * NT):
            part = x_ref[rows, n * TN:(n + 1) * TN].astype(F32)
            total = total + jnp.sum(part * part, axis=1, keepdims=True)
        inv = lax.rsqrt(total * (1.0 / WIDTH) + EPS)
        for n in range(2 * NT):
            cols = slice(n * TN, (n + 1) * TN)
            h_ref[rows, cols] = (x_ref[rows, cols].astype(F32) * inv * gain_row[0:1, cols]).astype(BF16)
        return 0

    lax.fori_loop(0, SEQS // 16, norm_step, 0)

    def slab(i, _):
        for copy in load_w(i):
            copy.wait()
        rows = pl.ds(pl.multiple_of(i * KS, KS), KS)
        for n in range(QKV // TN):
            cols = slice(n * TN, (n + 1) * TN)
            acc[:, cols] += jnp.dot(h_ref[:, rows], w_ref[rows, cols], preferred_element_type=F32)
        return 0

    lax.fori_loop(0, SLABS, slab, 0)

    def split(r, _):
        rows = pl.ds(pl.multiple_of(r * 32, 32), 32)
        cos_r = cos_ref[rows, :]
        sin_r = sin_ref[rows, :]

        def head(j):
            return acc[rows, j * HD:(j + 1) * HD].astype(BF16).astype(F32)

        def rotate(v):
            return (v * cos_r + pltpu.roll(v, HD // 2, 1) * sin_r).astype(BF16).astype(F32)

        for j in range(QH):
            q_ref[rows, j, :] = rotate(head(j))
        group = QH // KVH
        for j in range(KVH):
            key = rotate(head(QH + j))
            value = head(QH + KVH + j)
            kn_ref[rows, j, :] = key
            vn_ref[rows, j, :] = value
            for i in range(group):
                kx_ref[rows, j * group + i, :] = key
                vx_ref[rows, j * group + i, :] = value
        return 0

    lax.fori_loop(0, SEQS // 32, split, 0)
    spread_gain(gain2_ref, gain_row)
    pl.semaphore_wait(barrier, 2)

    def remote(src, dst, send, recv, device):
        return pltpu.make_async_remote_copy(src_ref=src, dst_ref=dst, send_sem=send, recv_sem=recv,
                                            device_id={"tp": device}, device_id_type=pl.DeviceIdType.MESH)

    def rows_of(c):
        return pl.ds(pl.multiple_of(c * ROWS, ROWS), ROWS)

    def send1(c):
        return remote(ybuf.at[other, :, rows_of(c)], rb1.at[:, rows_of(c)], s1.at[c], r1.at[c], partner)

    def send2(c):
        return remote(sb.at[:, rows_of(c)], rb2.at[:, rows_of(c)], s2.at[c], r2.at[c], peer)

    def send3(c):
        return remote(tb.at[mine, :, rows_of(c)], tb.at[mine, :, rows_of(c)], s3.at[c], r3.at[c], partner)

    def recv3(c):
        return remote(tb.at[other, :, rows_of(c)], tb.at[other, :, rows_of(c)], s3.at[c], r3.at[c], partner)

    col = lax.broadcasted_iota(jnp.int32, (QH, KVH * SLOTS), 1)
    row_head = lax.broadcasted_iota(jnp.int32, (QH, KVH * SLOTS), 0) // (QH // KVH)
    col_slot = jnp.where(lax.rem(col, KVH) == row_head, col // KVH, SLOTS)
    scale = 1.0 / math.sqrt(HD)

    def attend(g, base):
        slot = lax.rem(g, KVSLOTS)
        for copy in load_kv(g):
            copy.wait()
        qs = [q_ref[g * BLK + i] for i in range(BLK)]
        score = [lax.dot_general(qs[i].astype(BF16), kbuf[slot, i], (((1,), (1,)), ((), ())),
                                 preferred_element_type=F32) for i in range(BLK)]
        new = [jnp.sum(qs[i] * kx_ref[g * BLK + i], axis=1, keepdims=True) * scale for i in range(BLK)]
        score = [jnp.where(col_slot < pos_ref[g * BLK + i], score[i] * scale, -jnp.inf) for i in range(BLK)]
        top = [jnp.maximum(jnp.max(score[i], axis=1, keepdims=True), new[i]) for i in range(BLK)]
        e = [jnp.exp(score[i] - top[i]) for i in range(BLK)]
        e_new = [jnp.exp(new[i] - top[i]) for i in range(BLK)]
        inv = [1.0 / (jnp.sum(e[i], axis=1, keepdims=True) + e_new[i]) for i in range(BLK)]
        for i in range(BLK):
            prob = (e[i] * inv[i]).astype(BF16)
            prob_new = (e_new[i] * inv[i]).astype(BF16).astype(F32)
            out = jnp.dot(prob, vbuf[slot, i], preferred_element_type=F32)
            out = out + prob_new * vx_ref[g * BLK + i]
            o3[base + i] = out.astype(BF16).astype(F32)

        @pl.when(g + KVSLOTS < SEQS // BLK)
        def _():
            for copy in load_kv(g + KVSLOTS):
                copy.start()

    def project(c, half):
        for n in range(NT):
            ybuf[half, n, rows_of(c), :] = jnp.dot(o2[...], wo[half, :, n * TN:(n + 1) * TN],
                                                   preferred_element_type=F32)

    def stage2(c):
        send1(c).wait_recv()
        sb[:, rows_of(c)] = ybuf[mine, :, rows_of(c)] + rb1[:, rows_of(c)]
        send2(c).start()

    def stage3(c):
        send2(c).wait_recv()
        tb[mine, :, rows_of(c)] = sb[:, rows_of(c)] + rb2[:, rows_of(c)]
        send3(c).start()

    def stage4(c):
        recv3(c).wait_recv()

        def body(i, _):
            rows = pl.ds(pl.multiple_of(c * ROWS + i * 16, 16), 16)
            total = jnp.zeros((16, 1), F32)
            for half in range(2):
                for n in range(NT):
                    cols = slice(half * HALF + n * TN, half * HALF + (n + 1) * TN)
                    x1 = (x_ref[rows, cols].astype(F32) + tb[half, n, rows, :]).astype(BF16)
                    x1_ref[rows, cols] = x1
                    x1_f = x1.astype(F32)
                    total = total + jnp.sum(x1_f * x1_f, axis=1, keepdims=True)
            inv = lax.rsqrt(total * (1.0 / WIDTH) + EPS)
            for n in range(2 * NT):
                cols = slice(n * TN, (n + 1) * TN)
                h2[rows, cols] = (x1_ref[rows, cols].astype(F32) * inv * gain_row[0:1, cols]).astype(BF16)
            return 0

        lax.fori_loop(0, ROWS // 16, body, 0)

    def chunk(c, _):
        def block(j, _):
            attend(c * BLKS + j, j * BLK)

            @pl.when((j == 0) & (c >= 1))
            def _():
                stage2(c - 1)

            return 0

        lax.fori_loop(0, BLKS, block, 0)
        for j in range(QH):
            o2[:, j * HD:(j + 1) * HD] = o3[:, j, :].astype(BF16)

        @pl.when(c == 0)
        def _():
            for copy in load_wo:
                copy.wait()

        project(c, other)
        send1(c).start()
        project(c, mine)

        @pl.when(c >= 3)
        def _():
            stage3(c - 3)

        @pl.when(c >= 4)
        def _():
            stage4(c - 4)

        return 0

    lax.fori_loop(0, CHUNKS, chunk, 0)
    stage2(CHUNKS - 1)
    stage4(CHUNKS - 4)

    def tail(c, _):
        @pl.when(c < CHUNKS)
        def _():
            stage3(c)

        @pl.when(c > CHUNKS - 3)
        def _():
            stage4(c - 1)

        return 0

    lax.fori_loop(CHUNKS - 3, CHUNKS + 1, tail, 0)

    def sent(c, _):
        send1(c).wait_send()
        send2(c).wait_send()
        send3(c).wait_send()
        return 0

    lax.fori_loop(0, CHUNKS, sent, 0)


def attention(positions, cos_t, sin_t, gain1, gain2, resid_in, w_query, w_key, w_value, k_rows, v_rows, w_out):
    vmem = pl.BlockSpec(memory_space=pltpu.VMEM)
    hbm = pl.BlockSpec(memory_space=pl.ANY)
    dma = pltpu.SemaphoreType.DMA
    shape = jax.ShapeDtypeStruct
    return pl.pallas_call(
        attention_kernel,
        name="attention",
        out_shape=(shape((SEQS, WIDTH), BF16), shape((SEQS, WIDTH), BF16),
                   shape((SEQS, KVH, HD), F32), shape((SEQS, KVH, HD), F32)),
        in_specs=[pl.BlockSpec(memory_space=pltpu.SMEM)] + [vmem] * 4 + [hbm] * 7,
        out_specs=(vmem,) * 4,
        scratch_shapes=[
            pltpu.VMEM((SEQS, WIDTH), BF16), pltpu.VMEM((SEQS, WIDTH), BF16), pltpu.VMEM((WIDTH, QKV), BF16),
            pltpu.VMEM((SEQS, QKV), F32),
            pltpu.VMEM((SEQS, QH, HD), F32), pltpu.VMEM((SEQS, QH, HD), F32), pltpu.VMEM((SEQS, QH, HD), F32),
            pltpu.VMEM((8, WIDTH), F32),
            pltpu.VMEM((KVSLOTS, BLK, KVH * SLOTS, HD), BF16), pltpu.VMEM((KVSLOTS, BLK, KVH * SLOTS, HD), BF16),
            pltpu.VMEM((2, QH * HD, HALF), BF16),
            pltpu.VMEM((ROWS, QH, HD), F32), pltpu.VMEM((ROWS, QH * HD), BF16),
            pltpu.VMEM((2, NT, SEQS, TN), F32), pltpu.VMEM((NT, SEQS, TN), F32), pltpu.VMEM((NT, SEQS, TN), F32),
            pltpu.VMEM((NT, SEQS, TN), F32), pltpu.VMEM((2, NT, SEQS, TN), F32),
            dma, dma((SLABS,)), dma((SLABS,)), dma((SLABS,)), dma((KVSLOTS,)), dma((KVSLOTS,)), dma((2,)),
            dma((CHUNKS,)), dma((CHUNKS,)), dma((CHUNKS,)), dma((CHUNKS,)), dma((CHUNKS,)), dma((CHUNKS,))],
        compiler_params=pltpu.CompilerParams(collective_id=0, has_side_effects=True, vmem_limit_bytes=VMEM_ALL),
        cost_estimate=pl.CostEstimate(flops=10**10, bytes_accessed=100 * 2**20, transcendentals=0),
    )(positions, cos_t, sin_t, gain1, gain2, resid_in, w_query, w_key, w_value, k_rows, v_rows, w_out)


def mlp_kernel(h2, wg_hbm, wu_hbm, wd_hbm, z_ref, act, gbuf, wbuf, zs, zr, w_sem, s4, r4):
    tp = lax.axis_index("tp")
    mine = lax.rem(tp, 2)
    other = 1 - mine
    partner = tp + 1 - 2 * mine

    def load_gate(t, slot):
        cols = pl.ds(pl.multiple_of(t * TN, TN), TN)
        return pltpu.make_async_copy(wg_hbm.at[:, cols], wbuf.at[slot], w_sem.at[slot])

    def load_up(t, slot):
        cols = pl.ds(pl.multiple_of(t * TN, TN), TN)
        return pltpu.make_async_copy(wu_hbm.at[:, cols], wbuf.at[slot], w_sem.at[slot])

    def load_down(t, slot):
        if isinstance(t, int):
            t = jnp.int32(t)
        far = (t < NT).astype(jnp.int32)
        half = far * other + (1 - far) * mine
        start = half * HALF + (t - (1 - far) * NT) * TN
        cols = pl.ds(pl.multiple_of(start, TN), TN)
        return pltpu.make_async_copy(wd_hbm.at[:, cols], wbuf.at[slot, pl.ds(0, FFN)], w_sem.at[slot])

    def start_tile(i):
        slot = lax.rem(i, WSLOTS)
        odd = lax.rem(i, 2)

        @pl.when((i < 2 * GT) & (odd == 0))
        def _():
            load_gate(i // 2, slot).start()

        @pl.when((i < 2 * GT) & (odd == 1))
        def _():
            load_up(i // 2, slot).start()

        @pl.when((i >= 2 * GT) & (i < N_TILES))
        def _():
            load_down(i - 2 * GT, slot).start()

    def first(i, _):
        start_tile(i)
        return 0

    lax.fori_loop(0, WSLOTS, first, 0)
    barrier = pltpu.get_barrier_semaphore()
    pl.semaphore_signal(barrier, inc=1, device_id={"tp": partner}, device_id_type=pl.DeviceIdType.MESH)
    pl.semaphore_wait(barrier, 1)

    def mm(lhs_ref, slot, depth, n):
        return jnp.dot(lhs_ref[...], wbuf[slot, 0:depth, n * 256:(n + 1) * 256], preferred_element_type=F32)

    def gate_up(t, _):
        slot = lax.rem(2 * t, WSLOTS)
        load_gate(t, slot).wait()
        for n in range(TN // 256):
            gbuf[:, n * 256:(n + 1) * 256] = mm(h2, slot, WIDTH, n).astype(BF16)
        start_tile(2 * t + WSLOTS)
        slot = lax.rem(2 * t + 1, WSLOTS)
        load_up(t, slot).wait()
        for n in range(TN // 256):
            up = mm(h2, slot, WIDTH, n).astype(BF16).astype(F32)
            gate = gbuf[:, n * 256:(n + 1) * 256].astype(F32)
            act[:, pl.ds(pl.multiple_of(t * TN + n * 256, 256), 256)] = (jax.nn.silu(gate) * up).astype(BF16)
        start_tile(2 * t + 1 + WSLOTS)
        return 0

    lax.fori_loop(0, GT, gate_up, 0)

    def send4(t):
        return pltpu.make_async_remote_copy(src_ref=zs.at[t], dst_ref=zr.at[t], send_sem=s4.at[t], recv_sem=r4.at[t],
                                            device_id={"tp": partner}, device_id_type=pl.DeviceIdType.MESH)

    def down_far(t, _):
        i = 2 * GT + t
        slot = lax.rem(i, WSLOTS)
        load_down(t, slot).wait()
        for n in range(TN // 256):
            zs[t, :, n * 256:(n + 1) * 256] = mm(act, slot, FFN, n)
        send4(t).start()
        start_tile(i + WSLOTS)
        return 0

    lax.fori_loop(0, NT, down_far, 0)

    def down_near(t, _):
        i = 2 * GT + NT + t
        slot = lax.rem(i, WSLOTS)
        load_down(NT + t, slot).wait()
        send4(t).wait_recv()
        for n in range(TN // 256):
            z_ref[t, :, n * 256:(n + 1) * 256] = mm(act, slot, FFN, n) + zr[t, :, n * 256:(n + 1) * 256]
        start_tile(i + WSLOTS)
        return 0

    lax.fori_loop(0, NT, down_near, 0)

    def sent4(t, _):
        send4(t).wait_send()
        return 0

    lax.fori_loop(0, NT, sent4, 0)


def mlp(h2, w_gate, w_up, w_down):
    vmem = pl.BlockSpec(memory_space=pltpu.VMEM)
    hbm = pl.BlockSpec(memory_space=pl.ANY)
    dma = pltpu.SemaphoreType.DMA
    return pl.pallas_call(
        mlp_kernel,
        name="mlp",
        out_shape=jax.ShapeDtypeStruct((NT, SEQS, TN), F32),
        in_specs=[vmem] + [hbm] * 3,
        out_specs=vmem,
        scratch_shapes=[
            pltpu.VMEM((SEQS, FFN), BF16), pltpu.VMEM((SEQS, TN), BF16), pltpu.VMEM((WSLOTS, WIDTH, TN), BF16),
            pltpu.VMEM((NT, SEQS, TN), F32), pltpu.VMEM((NT, SEQS, TN), F32),
            dma((WSLOTS,)), dma((NT,)), dma((NT,))],
        compiler_params=pltpu.CompilerParams(collective_id=2, has_side_effects=True, vmem_limit_bytes=VMEM_ALL),
        cost_estimate=pl.CostEstimate(flops=2 * 10**10, bytes_accessed=90 * 2**20, transcendentals=0),
    )(h2, w_gate, w_up, w_down)


def final_kernel(z_ref, zr_ref, x1_ref, out_ref, tb, send_sem, recv_sem):
    tp = lax.axis_index("tp")
    mine = lax.rem(tp, 2)
    other = 1 - mine
    partner = tp + 1 - 2 * mine
    barrier = pltpu.get_barrier_semaphore()
    pl.semaphore_signal(barrier, inc=1, device_id={"tp": partner}, device_id_type=pl.DeviceIdType.MESH)
    pl.semaphore_wait(barrier, 1)

    def copy(half, t):
        return pltpu.make_async_remote_copy(src_ref=tb.at[half, t], dst_ref=tb.at[half, t], send_sem=send_sem.at[t],
                                            recv_sem=recv_sem.at[t], device_id={"tp": partner},
                                            device_id_type=pl.DeviceIdType.MESH)

    def add(half, t):
        cols = pl.ds(pl.multiple_of(half * HALF + t * TN, TN), TN)
        out_ref[:, cols] = (x1_ref[:, cols].astype(F32) + tb[half, t]).astype(BF16)

    for t in range(NT):
        tb[mine, t] = z_ref[t] + zr_ref[t]
        copy(mine, t).start()
    for t in range(NT):
        add(mine, t)
    for t in range(NT):
        copy(other, t).wait_recv()
        add(other, t)
    for t in range(NT):
        copy(mine, t).wait_send()


def finish(z, z_peer, x1):
    vmem = pl.BlockSpec(memory_space=pltpu.VMEM)
    return pl.pallas_call(
        final_kernel,
        name="finish",
        out_shape=jax.ShapeDtypeStruct((SEQS, WIDTH), BF16),
        in_specs=[vmem] * 3,
        out_specs=vmem,
        scratch_shapes=[pltpu.VMEM((2, NT, SEQS, TN), F32), pltpu.SemaphoreType.DMA((NT,)),
                        pltpu.SemaphoreType.DMA((NT,))],
        compiler_params=pltpu.CompilerParams(collective_id=1, has_side_effects=True, vmem_limit_bytes=24 * 2**20),
        cost_estimate=pl.CostEstimate(flops=2 * 10**8, bytes_accessed=10 * 2**20, transcendentals=0),
    )(z, z_peer, x1)


def solution(mesh):
    def layer_local(resid_in, positions, k_cache, v_cache, gain_attn, w_query, w_key, w_value,
                    w_out, gain_mlp, w_gate, w_up, w_down):
        cos_t, sin_t = rope_tables(positions, HD)
        k_rows = k_cache.reshape(SEQS, SLOTS * KVH, HD)
        v_rows = v_cache.reshape(SEQS, SLOTS * KVH, HD)
        x1, h2, kn, vn = attention(positions, cos_t, sin_t, gain_attn.reshape(32, 128), gain_mlp.reshape(32, 128),
                                   resid_in, w_query, w_key, w_value, k_rows, v_rows, w_out)
        z = mlp(h2, w_gate, w_up, w_down)
        z_peer = lax.ppermute(z, 'tp', [(0, 2), (1, 3), (2, 0), (3, 1)])
        k_full, v_full = write_caches(positions, kn, vn, k_cache, v_cache, z)
        resid_out = finish(z, z_peer, x1)
        return resid_out, k_full, v_full

    row_spec = P('dp', None)
    cache_spec = P('dp', None, 'tp', None)
    col_spec = P(None, 'tp')
    split_rows = P('tp', None)
    return jax.shard_map(layer_local, mesh=mesh,
                         in_specs=(row_spec, P('dp'), cache_spec, cache_spec, P(), col_spec, col_spec,
                                   col_spec, split_rows, P(), col_spec, col_spec, split_rows),
                         out_specs=(row_spec, cache_spec, cache_spec), check_vma=False)
```

```python
import functools
import math
import jax
import jax.numpy as jnp
from jax import lax
from jax.experimental import pallas as pl
from jax.experimental.pallas import tpu as pltpu
from jax.sharding import PartitionSpec as P

EPS = 1e-5
ROPE_THETA = 500000.0
ROPE_FACTOR = 8.0
LOW_FACTOR = 1.0
HIGH_FACTOR = 4.0
ORIG_CTX = 8192.0

F32 = jnp.float32
BF16 = jnp.bfloat16
SEQS = 256
SLOTS = 256
WIDTH = 4096
HALF = WIDTH // 2
HD = 128
QH = 8
KVH = 2
FFN = 3584
VMEM_ALL = 67043328

ROWS = 32
CHUNKS = SEQS // ROWS
BLK = 8
BLKS = ROWS // BLK
KVSLOTS = 3
TN = 512
NT = HALF // TN
WSLOTS = 5
GT = FFN // TN
N_TILES = 2 * GT + 2 * NT


def rope_tables(positions, head_dim):
    half_dim = head_dim // 2
    lane = jnp.arange(head_dim)
    exponents = (lane % half_dim).astype(jnp.float32) * (2.0 / head_dim)
    inv_freq = 1.0 / jnp.power(ROPE_THETA, exponents)
    wavelen = (2.0 * math.pi) / inv_freq
    smooth = (ORIG_CTX / wavelen - LOW_FACTOR) / (HIGH_FACTOR - LOW_FACTOR)
    blended = (1.0 - smooth) * inv_freq / ROPE_FACTOR + smooth * inv_freq
    inv_freq = jnp.where(wavelen < ORIG_CTX / HIGH_FACTOR, inv_freq,
                         jnp.where(wavelen > ORIG_CTX / LOW_FACTOR, inv_freq / ROPE_FACTOR, blended))
    angles = positions[:, None].astype(jnp.float32) * inv_freq[None, :]
    sign = jnp.where(lane < half_dim, -1.0, 1.0).astype(jnp.float32)
    return jnp.cos(angles), jnp.sin(angles) * sign[None, :]


CBLK = 8
CSLOTS = 24


def cache_kernel(pos_ref, kn_ref, vn_ref, k_hbm, v_hbm, after_hbm, k_out, v_out, buf, in_sem, out_sem):
    steps = [(src, dst, new, i) for i in range(SEQS // CBLK)
             for src, dst, new in ((k_hbm, k_out, kn_ref), (v_hbm, v_out, vn_ref))]
    n = len(steps)
    ahead = CSLOTS // 2

    def load(s):
        src, _, _, i = steps[s]
        return pltpu.make_async_copy(src.at[pl.ds(i * CBLK, CBLK)], buf.at[s % CSLOTS], in_sem.at[s % CSLOTS])

    def save(s):
        _, dst, _, i = steps[s]
        return pltpu.make_async_copy(buf.at[s % CSLOTS], dst.at[pl.ds(i * CBLK, CBLK)], out_sem.at[s % CSLOTS])

    for s in range(ahead):
        load(s).start()
    for s in range(n):
        if s + ahead < n:
            if s + ahead >= CSLOTS:
                save(s + ahead - CSLOTS).wait()
            load(s + ahead).start()
        load(s).wait()
        _, _, new, i = steps[s]

        def patch(j, _, new=new, i=i, s=s):
            row = i * CBLK + j
            pair = jnp.concatenate([new[h, pl.ds(row, 1), :] for h in range(KVH)], axis=0)
            buf[s % CSLOTS, j, pos_ref[row]] = pair.astype(BF16)
            return 0

        lax.fori_loop(0, CBLK, patch, 0)
        save(s).start()
    for s in range(n - CSLOTS, n):
        save(s).wait()


def write_caches(positions, kn, vn, k_cache, v_cache, after):
    vmem = pl.BlockSpec(memory_space=pltpu.VMEM)
    hbm = pl.BlockSpec(memory_space=pl.ANY)
    cache = jax.ShapeDtypeStruct(k_cache.shape, BF16)
    return pl.pallas_call(
        cache_kernel,
        name="write_caches",
        out_shape=(cache, cache),
        in_specs=[pl.BlockSpec(memory_space=pltpu.SMEM), vmem, vmem, hbm, hbm, hbm],
        out_specs=(hbm, hbm),
        scratch_shapes=[pltpu.VMEM((CSLOTS, CBLK, SLOTS, KVH, HD), BF16),
                        pltpu.SemaphoreType.DMA((CSLOTS,)), pltpu.SemaphoreType.DMA((CSLOTS,))],
        compiler_params=pltpu.CompilerParams(vmem_limit_bytes=56 * 2**20),
        cost_estimate=pl.CostEstimate(flops=2 * 10**10, bytes_accessed=128 * 2**20, transcendentals=0),
    )(positions, kn, vn, k_cache, v_cache, after)


KS = 512
SLABS = WIDTH // KS
PITCH = 264
QKV = (QH + 2 * KVH) * HD


def spread_gain(gain_ref, gain_row):
    for n in range(WIDTH // 128):
        gain_row[:, n * 128:(n + 1) * 128] = jnp.broadcast_to(gain_ref[n:n + 1, :].astype(F32), (8, 128))


def layer_kernel(pos_hbm, cos_hbm, sin_hbm, gain1_hbm, gain2_hbm, x_hbm, wq_hbm, wk_hbm, wv_hbm, k_hbm, v_hbm,
                 wo_hbm, wg_hbm, wu_hbm, wd_hbm, x1_hbm, z_hbm, kn_ref, vn_ref,
                 pos_ref, cos_ref, sin_ref, gain1_ref, gain2_ref, x_ref, x1_ref, h2, q_ref, gain_row,
                 kbuf, vbuf, wo, o3, o2, ybuf, rb1, sb, rb2, tb, act, gbuf, wbuf,
                 small_sem, x_sem, q_sem, k_sem, v_sem, kc_sem, vc_sem, wo_sem, w_sem, x1_sem, z_sem,
                 s1, r1, s2, r2, s3, r3, s4, r4):
    tp = lax.axis_index("tp")
    mine = lax.rem(tp, 2)
    other = 1 - mine
    partner = tp + 1 - 2 * mine
    peer = lax.rem(tp + 2, 4)

    load_x = pltpu.make_async_copy(x_hbm, x_ref, x_sem)
    load_x.start()
    small = [pltpu.make_async_copy(src, dst, small_sem.at[i]) for i, (src, dst) in enumerate(
        ((gain1_hbm, gain1_ref), (gain2_hbm, gain2_ref), (cos_hbm, cos_ref), (sin_hbm, sin_ref), (pos_hbm, pos_ref)))]
    for copy in small:
        copy.start()

    def load_w(i):
        rows = pl.ds(i * KS, KS)
        kv = KVH * HD
        return (pltpu.make_async_copy(wq_hbm.at[rows, pl.ds(0, TN)], wbuf.at[0, rows], q_sem.at[0, i]),
                pltpu.make_async_copy(wq_hbm.at[rows, pl.ds(TN, TN)], wbuf.at[1, rows], q_sem.at[1, i]),
                pltpu.make_async_copy(wk_hbm.at[rows], wbuf.at[2, rows, pl.ds(0, kv)], k_sem.at[i]),
                pltpu.make_async_copy(wv_hbm.at[rows], wbuf.at[2, rows, pl.ds(kv, kv)], v_sem.at[i]))

    for i in range(SLABS):
        for copy in load_w(i):
            copy.start()

    def load_kv(g):
        slot = lax.rem(g, KVSLOTS)
        seqs = pl.ds(g * BLK, BLK)
        return (pltpu.make_async_copy(k_hbm.at[seqs], kbuf.at[slot], kc_sem.at[slot]),
                pltpu.make_async_copy(v_hbm.at[seqs], vbuf.at[slot], vc_sem.at[slot]))

    for g in range(2):
        for copy in load_kv(g):
            copy.start()
    load_wo = [pltpu.make_async_copy(wo_hbm.at[:, pl.ds(i * HALF, HALF)], wo.at[i], wo_sem.at[i]) for i in range(2)]
    for copy in load_wo:
        copy.start()
    for g in range(2, KVSLOTS):
        for copy in load_kv(g):
            copy.start()

    barrier = pltpu.get_barrier_semaphore()
    for device in (partner, peer):
        pl.semaphore_signal(barrier, inc=1, device_id={"tp": device}, device_id_type=pl.DeviceIdType.MESH)

    for n in range(QKV // TN):
        ybuf[0, n] = jnp.zeros((SEQS, TN), F32)
    for copy in small:
        copy.wait()
    spread_gain(gain1_ref, gain_row)
    load_x.wait()

    def norm_step(i, _):
        rows = pl.ds(pl.multiple_of(i * 16, 16), 16)
        total = jnp.zeros((16, 1), F32)
        for n in range(2 * NT):
            part = x_ref[rows, n * TN:(n + 1) * TN].astype(F32)
            total = total + jnp.sum(part * part, axis=1, keepdims=True)
        inv = lax.rsqrt(total * (1.0 / WIDTH) + EPS)
        for n in range(2 * NT):
            cols = slice(n * TN, (n + 1) * TN)
            h2[rows, cols] = (x_ref[rows, cols].astype(F32) * inv * gain_row[0:1, cols]).astype(BF16)
        return 0

    lax.fori_loop(0, SEQS // 16, norm_step, 0)

    def slab(i, _):
        for copy in load_w(i):
            copy.wait()
        rows = pl.ds(pl.multiple_of(i * KS, KS), KS)
        for n in range(QKV // TN):
            ybuf[0, n] += jnp.dot(h2[:, rows], wbuf[n, rows, :], preferred_element_type=F32)
        return 0

    lax.fori_loop(0, SLABS, slab, 0)

    def split(r, _):
        rows = pl.ds(pl.multiple_of(r * 32, 32), 32)
        cos_r = cos_ref[rows, :]
        sin_r = sin_ref[rows, :]

        def head(j):
            per = TN // HD
            return ybuf[0, j // per, rows, (j % per) * HD:(j % per + 1) * HD].astype(BF16).astype(F32)

        def rotate(v):
            return (v * cos_r + pltpu.roll(v, HD // 2, 1) * sin_r).astype(BF16).astype(F32)

        for j in range(QH):
            q_ref[pl.ds(pl.multiple_of(j * PITCH + r * 32, 8), 32), :] = rotate(head(j))
        for j in range(KVH):
            kn_ref[j, rows, :] = rotate(head(QH + j))
            vn_ref[j, rows, :] = head(QH + KVH + j)
        return 0

    lax.fori_loop(0, SEQS // 32, split, 0)
    spread_gain(gain2_ref, gain_row)
    pl.semaphore_wait(barrier, 2)

    def remote(src, dst, send, recv, device):
        return pltpu.make_async_remote_copy(src_ref=src, dst_ref=dst, send_sem=send, recv_sem=recv,
                                            device_id={"tp": device}, device_id_type=pl.DeviceIdType.MESH)

    def rows_of(c):
        return pl.ds(pl.multiple_of(c * ROWS, ROWS), ROWS)

    def send1(c):
        return remote(ybuf.at[other, :, rows_of(c)], rb1.at[:, rows_of(c)], s1.at[c], r1.at[c], partner)

    def send2(c):
        return remote(sb.at[:, rows_of(c)], rb2.at[:, rows_of(c)], s2.at[c], r2.at[c], peer)

    def send3(c):
        return remote(tb.at[mine, :, rows_of(c)], tb.at[mine, :, rows_of(c)], s3.at[c], r3.at[c], partner)

    def recv3(c):
        return remote(tb.at[other, :, rows_of(c)], tb.at[other, :, rows_of(c)], s3.at[c], r3.at[c], partner)

    def load_gate(t, slot):
        cols = pl.ds(pl.multiple_of(t * TN, TN), TN)
        return pltpu.make_async_copy(wg_hbm.at[:, cols], wbuf.at[slot], w_sem.at[slot])

    def load_up(t, slot):
        cols = pl.ds(pl.multiple_of(t * TN, TN), TN)
        return pltpu.make_async_copy(wu_hbm.at[:, cols], wbuf.at[slot], w_sem.at[slot])

    def load_down(t, slot):
        if isinstance(t, int):
            t = jnp.int32(t)
        far = (t < NT).astype(jnp.int32)
        half = far * other + (1 - far) * mine
        start = half * HALF + (t - (1 - far) * NT) * TN
        cols = pl.ds(pl.multiple_of(start, TN), TN)
        return pltpu.make_async_copy(wd_hbm.at[:, cols], wbuf.at[slot, pl.ds(0, FFN)], w_sem.at[slot])

    def start_tile(i):
        slot = lax.rem(i, WSLOTS)
        odd = lax.rem(i, 2)

        @pl.when((i < 2 * GT) & (odd == 0))
        def _():
            load_gate(i // 2, slot).start()

        @pl.when((i < 2 * GT) & (odd == 1))
        def _():
            load_up(i // 2, slot).start()

        @pl.when((i >= 2 * GT) & (i < N_TILES))
        def _():
            load_down(i - 2 * GT, slot).start()

    col = lax.broadcasted_iota(jnp.int32, (QH, KVH * SLOTS), 1)
    row_head = lax.broadcasted_iota(jnp.int32, (QH, KVH * SLOTS), 0) // (QH // KVH)
    col_slot = jnp.where(lax.rem(col, KVH) == row_head, col // KVH, SLOTS)
    scale = 1.0 / math.sqrt(HD)
    low = lax.broadcasted_iota(jnp.int32, (QH, HD), 0) < QH // KVH

    def by_head(ref, b):
        return jnp.where(low, ref[0, pl.ds(b, 1), :], ref[1, pl.ds(b, 1), :])

    def attend(g, base):
        slot = lax.rem(g, KVSLOTS)
        for copy in load_kv(g):
            copy.wait()
        qs = [q_ref[pl.ds(g * BLK + i, QH, stride=PITCH), :] for i in range(BLK)]
        score = [lax.dot_general(qs[i].astype(BF16), kbuf[slot, i], (((1,), (1,)), ((), ())),
                                 preferred_element_type=F32) for i in range(BLK)]
        new = [jnp.sum(qs[i] * by_head(kn_ref, g * BLK + i), axis=1, keepdims=True) * scale for i in range(BLK)]
        score = [jnp.where(col_slot < pos_ref[g * BLK + i], score[i] * scale, -jnp.inf) for i in range(BLK)]
        top = [jnp.maximum(jnp.max(score[i], axis=1, keepdims=True), new[i]) for i in range(BLK)]
        e = [jnp.exp(score[i] - top[i]) for i in range(BLK)]
        e_new = [jnp.exp(new[i] - top[i]) for i in range(BLK)]
        inv = [1.0 / (jnp.sum(e[i], axis=1, keepdims=True) + e_new[i]) for i in range(BLK)]
        for i in range(BLK):
            prob = (e[i] * inv[i]).astype(BF16)
            prob_new = (e_new[i] * inv[i]).astype(BF16).astype(F32)
            out = jnp.dot(prob, vbuf[slot, i], preferred_element_type=F32)
            out = out + prob_new * by_head(vn_ref, g * BLK + i)
            o3[base + i] = out.astype(BF16).astype(F32)

        @pl.when(g + KVSLOTS < SEQS // BLK)
        def _():
            for copy in load_kv(g + KVSLOTS):
                copy.start()

    def project(c, half):
        for n in range(NT):
            ybuf[half, n, rows_of(c), :] = jnp.dot(o2[...], wo[half, :, n * TN:(n + 1) * TN],
                                                   preferred_element_type=F32)

    def stage2(c):
        send1(c).wait_recv()
        sb[:, rows_of(c)] = ybuf[mine, :, rows_of(c)] + rb1[:, rows_of(c)]
        send2(c).start()

    def stage3(c):
        send2(c).wait_recv()
        tb[mine, :, rows_of(c)] = sb[:, rows_of(c)] + rb2[:, rows_of(c)]
        send3(c).start()

    def stage4(c):
        recv3(c).wait_recv()

        def body(i, _):
            rows = pl.ds(pl.multiple_of(c * ROWS + i * 16, 16), 16)
            total = jnp.zeros((16, 1), F32)
            for half in range(2):
                for n in range(NT):
                    cols = slice(half * HALF + n * TN, half * HALF + (n + 1) * TN)
                    x1 = (x_ref[rows, cols].astype(F32) + tb[half, n, rows, :]).astype(BF16)
                    x1_ref[rows, cols] = x1
                    x1_f = x1.astype(F32)
                    total = total + jnp.sum(x1_f * x1_f, axis=1, keepdims=True)
            inv = lax.rsqrt(total * (1.0 / WIDTH) + EPS)
            for n in range(2 * NT):
                cols = slice(n * TN, (n + 1) * TN)
                h2[rows, cols] = (x1_ref[rows, cols].astype(F32) * inv * gain_row[0:1, cols]).astype(BF16)
            return 0

        lax.fori_loop(0, ROWS // 16, body, 0)

    def chunk(c, _):
        def block(j, _):
            attend(c * BLKS + j, j * BLK)

            @pl.when((j == 0) & (c >= 1))
            def _():
                stage2(c - 1)

            return 0

        lax.fori_loop(0, BLKS, block, 0)
        for j in range(QH):
            o2[:, j * HD:(j + 1) * HD] = o3[:, j, :].astype(BF16)

        @pl.when(c == 0)
        def _():
            for copy in load_wo:
                copy.wait()

        project(c, other)
        send1(c).start()
        project(c, mine)

        @pl.when(c >= CHUNKS - WSLOTS)
        def _():
            start_tile(c - (CHUNKS - WSLOTS))

        @pl.when(c >= 3)
        def _():
            stage3(c - 3)

        @pl.when(c >= 4)
        def _():
            stage4(c - 4)

        return 0

    lax.fori_loop(0, CHUNKS, chunk, 0)
    stage2(CHUNKS - 1)
    stage4(CHUNKS - 4)

    def tail(c, _):
        @pl.when(c < CHUNKS)
        def _():
            stage3(c)

        @pl.when(c > CHUNKS - 3)
        def _():
            stage4(c - 1)

        return 0

    lax.fori_loop(CHUNKS - 3, CHUNKS + 1, tail, 0)

    def sent(c, _):
        send1(c).wait_send()
        send2(c).wait_send()
        send3(c).wait_send()
        return 0

    lax.fori_loop(0, CHUNKS, sent, 0)

    save_x1 = pltpu.make_async_copy(x1_ref, x1_hbm, x1_sem)
    save_x1.start()

    def mm(lhs_ref, slot, depth, n):
        return jnp.dot(lhs_ref[...], wbuf[slot, 0:depth, n * 256:(n + 1) * 256], preferred_element_type=F32)

    def gate_up(t, _):
        slot = lax.rem(2 * t, WSLOTS)
        load_gate(t, slot).wait()
        for n in range(TN // 256):
            gbuf[:, n * 256:(n + 1) * 256] = mm(h2, slot, WIDTH, n).astype(BF16)
        start_tile(2 * t + WSLOTS)
        slot = lax.rem(2 * t + 1, WSLOTS)
        load_up(t, slot).wait()
        for n in range(TN // 256):
            up = mm(h2, slot, WIDTH, n).astype(BF16).astype(F32)
            gate = gbuf[:, n * 256:(n + 1) * 256].astype(F32)
            act[:, pl.ds(pl.multiple_of(t * TN + n * 256, 256), 256)] = (jax.nn.silu(gate) * up).astype(BF16)
        start_tile(2 * t + 1 + WSLOTS)
        return 0

    lax.fori_loop(0, GT, gate_up, 0)

    def send4(t):
        return remote(ybuf.at[other, t], rb1.at[t], s4.at[t], r4.at[t], partner)

    def save_z(t):
        return pltpu.make_async_copy(sb.at[t], z_hbm.at[t], z_sem.at[t])

    def down_far(t, _):
        i = 2 * GT + t
        slot = lax.rem(i, WSLOTS)
        load_down(t, slot).wait()
        for n in range(TN // 256):
            ybuf[other, t, :, n * 256:(n + 1) * 256] = mm(act, slot, FFN, n)
        send4(t).start()
        start_tile(i + WSLOTS)
        return 0

    lax.fori_loop(0, NT, down_far, 0)

    def down_near(t, _):
        i = 2 * GT + NT + t
        slot = lax.rem(i, WSLOTS)
        load_down(NT + t, slot).wait()
        send4(t).wait_recv()
        for n in range(TN // 256):
            sb[t, :, n * 256:(n + 1) * 256] = mm(act, slot, FFN, n) + rb1[t, :, n * 256:(n + 1) * 256]
        save_z(t).start()
        start_tile(i + WSLOTS)
        return 0

    lax.fori_loop(0, NT, down_near, 0)

    def sent4(t, _):
        send4(t).wait_send()
        save_z(t).wait()
        return 0

    lax.fori_loop(0, NT, sent4, 0)
    save_x1.wait()


def layer(positions, cos_t, sin_t, gain1, gain2, resid_in, w_query, w_key, w_value, k_rows, v_rows, w_out,
          w_gate, w_up, w_down):
    vmem = pl.BlockSpec(memory_space=pltpu.VMEM)
    hbm = pl.BlockSpec(memory_space=pl.ANY)
    dma = pltpu.SemaphoreType.DMA
    shape = jax.ShapeDtypeStruct
    tile = (NT, SEQS, TN)
    return pl.pallas_call(
        layer_kernel,
        name="layer",
        out_shape=(shape((SEQS, WIDTH), BF16), shape(tile, F32),
                   shape((KVH, SEQS, HD), F32), shape((KVH, SEQS, HD), F32)),
        in_specs=[hbm] * 15,
        out_specs=(hbm, hbm, vmem, vmem),
        scratch_shapes=[
            pltpu.SMEM((SEQS,), jnp.int32), pltpu.VMEM((SEQS, HD), F32), pltpu.VMEM((SEQS, HD), F32),
            pltpu.VMEM((32, 128), BF16), pltpu.VMEM((32, 128), BF16),
            pltpu.VMEM((SEQS, WIDTH), BF16), pltpu.VMEM((SEQS, WIDTH), BF16), pltpu.VMEM((SEQS, WIDTH), BF16),
            pltpu.VMEM((QH * PITCH, HD), F32), pltpu.VMEM((8, WIDTH), F32),
            pltpu.VMEM((KVSLOTS, BLK, KVH * SLOTS, HD), BF16), pltpu.VMEM((KVSLOTS, BLK, KVH * SLOTS, HD), BF16),
            pltpu.VMEM((2, QH * HD, HALF), BF16),
            pltpu.VMEM((ROWS, QH, HD), F32), pltpu.VMEM((ROWS, QH * HD), BF16),
            pltpu.VMEM((2,) + tile, F32), pltpu.VMEM(tile, F32), pltpu.VMEM(tile, F32),
            pltpu.VMEM(tile, F32), pltpu.VMEM((2,) + tile, F32),
            pltpu.VMEM((SEQS, FFN), BF16), pltpu.VMEM((SEQS, TN), BF16), pltpu.VMEM((WSLOTS, WIDTH, TN), BF16),
            dma((5,)), dma, dma((2, SLABS)), dma((SLABS,)), dma((SLABS,)), dma((KVSLOTS,)), dma((KVSLOTS,)),
            dma((2,)), dma((WSLOTS,)), dma, dma((NT,)),
            dma((CHUNKS,)), dma((CHUNKS,)), dma((CHUNKS,)), dma((CHUNKS,)), dma((CHUNKS,)), dma((CHUNKS,)),
            dma((NT,)), dma((NT,))],
        compiler_params=pltpu.CompilerParams(collective_id=0, has_side_effects=True, vmem_limit_bytes=VMEM_ALL),
        cost_estimate=pl.CostEstimate(flops=3 * 10**10, bytes_accessed=190 * 2**20, transcendentals=0),
    )(positions, cos_t, sin_t, gain1, gain2, resid_in, w_query, w_key, w_value, k_rows, v_rows, w_out,
      w_gate, w_up, w_down)


def final_kernel(z_ref, zr_ref, x1_ref, out_ref, tb, send_sem, recv_sem):
    tp = lax.axis_index("tp")
    mine = lax.rem(tp, 2)
    other = 1 - mine
    partner = tp + 1 - 2 * mine
    barrier = pltpu.get_barrier_semaphore()
    pl.semaphore_signal(barrier, inc=1, device_id={"tp": partner}, device_id_type=pl.DeviceIdType.MESH)
    pl.semaphore_wait(barrier, 1)

    def copy(half, t):
        return pltpu.make_async_remote_copy(src_ref=tb.at[half, t], dst_ref=tb.at[half, t], send_sem=send_sem.at[t],
                                            recv_sem=recv_sem.at[t], device_id={"tp": partner},
                                            device_id_type=pl.DeviceIdType.MESH)

    def add(half, t):
        cols = pl.ds(pl.multiple_of(half * HALF + t * TN, TN), TN)
        out_ref[:, cols] = (x1_ref[:, cols].astype(F32) + tb[half, t]).astype(BF16)

    for t in range(NT):
        tb[mine, t] = z_ref[t] + zr_ref[t]
        copy(mine, t).start()
    for t in range(NT):
        add(mine, t)
    for t in range(NT):
        copy(other, t).wait_recv()
        add(other, t)
    for t in range(NT):
        copy(mine, t).wait_send()


def finish(z, z_peer, x1):
    vmem = pl.BlockSpec(memory_space=pltpu.VMEM)
    return pl.pallas_call(
        final_kernel,
        name="finish",
        out_shape=jax.ShapeDtypeStruct((SEQS, WIDTH), BF16),
        in_specs=[vmem] * 3,
        out_specs=vmem,
        scratch_shapes=[pltpu.VMEM((2, NT, SEQS, TN), F32), pltpu.SemaphoreType.DMA((NT,)),
                        pltpu.SemaphoreType.DMA((NT,))],
        compiler_params=pltpu.CompilerParams(collective_id=1, has_side_effects=True, vmem_limit_bytes=24 * 2**20),
        cost_estimate=pl.CostEstimate(flops=2 * 10**8, bytes_accessed=10 * 2**20, transcendentals=0),
    )(z, z_peer, x1)


def solution(mesh):
    def layer_local(resid_in, positions, k_cache, v_cache, gain_attn, w_query, w_key, w_value,
                    w_out, gain_mlp, w_gate, w_up, w_down):
        cos_t, sin_t = rope_tables(positions, HD)
        k_rows = k_cache.reshape(SEQS, SLOTS * KVH, HD)
        v_rows = v_cache.reshape(SEQS, SLOTS * KVH, HD)
        x1, z, kn, vn = layer(positions, cos_t, sin_t, gain_attn.reshape(32, 128), gain_mlp.reshape(32, 128),
                              resid_in, w_query, w_key, w_value, k_rows, v_rows, w_out, w_gate, w_up, w_down)
        z_peer = lax.ppermute(z, 'tp', [(0, 2), (1, 3), (2, 0), (3, 1)])
        k_full, v_full = write_caches(positions, kn, vn, k_cache, v_cache, z)
        resid_out = finish(z, z_peer, x1)
        return resid_out, k_full, v_full

    row_spec = P('dp', None)
    cache_spec = P('dp', None, 'tp', None)
    col_spec = P(None, 'tp')
    split_rows = P('tp', None)
    return jax.shard_map(layer_local, mesh=mesh,
                         in_specs=(row_spec, P('dp'), cache_spec, cache_spec, P(), col_spec, col_spec,
                                   col_spec, split_rows, P(), col_spec, col_spec, split_rows),
                         out_specs=(row_spec, cache_spec, cache_spec), check_vma=False)
```

```python
import functools
import math
import jax
import jax.numpy as jnp
from jax import lax
from jax.experimental import pallas as pl
from jax.experimental.pallas import tpu as pltpu
from jax.sharding import PartitionSpec as P

EPS = 1e-5
ROPE_THETA = 500000.0
ROPE_FACTOR = 8.0
LOW_FACTOR = 1.0
HIGH_FACTOR = 4.0
ORIG_CTX = 8192.0

F32 = jnp.float32
BF16 = jnp.bfloat16
SEQS = 256
SLOTS = 256
WIDTH = 4096
HALF = WIDTH // 2
HD = 128
QH = 8
KVH = 2
FFN = 3584
VMEM_ALL = 67043328

ROWS = 32
CHUNKS = SEQS // ROWS
BLK = 8
BLKS = ROWS // BLK
KVSLOTS = 3
TN = 512
NT = HALF // TN
WSLOTS = 5
GT = FFN // TN
N_TILES = 2 * GT + 2 * NT
PIECE = 64
PIECES = NT * SEQS // PIECE
PER = SEQS // PIECE
EARLY = 2


def rope_tables(positions, head_dim):
    half_dim = head_dim // 2
    lane = jnp.arange(head_dim)
    exponents = (lane % half_dim).astype(jnp.float32) * (2.0 / head_dim)
    inv_freq = 1.0 / jnp.power(ROPE_THETA, exponents)
    wavelen = (2.0 * math.pi) / inv_freq
    smooth = (ORIG_CTX / wavelen - LOW_FACTOR) / (HIGH_FACTOR - LOW_FACTOR)
    blended = (1.0 - smooth) * inv_freq / ROPE_FACTOR + smooth * inv_freq
    inv_freq = jnp.where(wavelen < ORIG_CTX / HIGH_FACTOR, inv_freq,
                         jnp.where(wavelen > ORIG_CTX / LOW_FACTOR, inv_freq / ROPE_FACTOR, blended))
    angles = positions[:, None].astype(jnp.float32) * inv_freq[None, :]
    sign = jnp.where(lane < half_dim, -1.0, 1.0).astype(jnp.float32)
    return jnp.cos(angles), jnp.sin(angles) * sign[None, :]


CBLK = 8
CSLOTS = 24


def cache_kernel(pos_ref, kn_ref, vn_ref, k_hbm, v_hbm, after_hbm, k_out, v_out, buf, in_sem, out_sem):
    steps = [(src, dst, new, i) for i in range(SEQS // CBLK)
             for src, dst, new in ((k_hbm, k_out, kn_ref), (v_hbm, v_out, vn_ref))]
    n = len(steps)
    ahead = CSLOTS // 2

    def load(s):
        src, _, _, i = steps[s]
        return pltpu.make_async_copy(src.at[pl.ds(i * CBLK, CBLK)], buf.at[s % CSLOTS], in_sem.at[s % CSLOTS])

    def save(s):
        _, dst, _, i = steps[s]
        return pltpu.make_async_copy(buf.at[s % CSLOTS], dst.at[pl.ds(i * CBLK, CBLK)], out_sem.at[s % CSLOTS])

    for s in range(ahead):
        load(s).start()
    for s in range(n):
        if s + ahead < n:
            if s + ahead >= CSLOTS:
                save(s + ahead - CSLOTS).wait()
            load(s + ahead).start()
        load(s).wait()
        _, _, new, i = steps[s]

        def patch(j, _, new=new, i=i, s=s):
            row = i * CBLK + j
            pair = jnp.concatenate([new[h, pl.ds(row, 1), :] for h in range(KVH)], axis=0)
            buf[s % CSLOTS, j, pos_ref[row]] = pair.astype(BF16)
            return 0

        lax.fori_loop(0, CBLK, patch, 0)
        save(s).start()
    for s in range(n - CSLOTS, n):
        save(s).wait()


def write_caches(positions, kn, vn, k_cache, v_cache, after):
    vmem = pl.BlockSpec(memory_space=pltpu.VMEM)
    hbm = pl.BlockSpec(memory_space=pl.ANY)
    cache = jax.ShapeDtypeStruct(k_cache.shape, BF16)
    return pl.pallas_call(
        cache_kernel,
        name="write_caches",
        out_shape=(cache, cache),
        in_specs=[pl.BlockSpec(memory_space=pltpu.SMEM), vmem, vmem, hbm, hbm, hbm],
        out_specs=(hbm, hbm),
        scratch_shapes=[pltpu.VMEM((CSLOTS, CBLK, SLOTS, KVH, HD), BF16),
                        pltpu.SemaphoreType.DMA((CSLOTS,)), pltpu.SemaphoreType.DMA((CSLOTS,))],
        compiler_params=pltpu.CompilerParams(vmem_limit_bytes=56 * 2**20),
        cost_estimate=pl.CostEstimate(flops=2 * 10**10, bytes_accessed=128 * 2**20, transcendentals=0),
    )(positions, kn, vn, k_cache, v_cache, after)


KS = 512
SLABS = WIDTH // KS
PITCH = 264
QKV = (QH + 2 * KVH) * HD


def spread_gain(gain_ref, gain_row):
    for n in range(WIDTH // 128):
        gain_row[:, n * 128:(n + 1) * 128] = jnp.broadcast_to(gain_ref[n:n + 1, :].astype(F32), (8, 128))


def layer_kernel(pos_hbm, cos_hbm, sin_hbm, gain1_hbm, gain2_hbm, x_hbm, wq_hbm, wk_hbm, wv_hbm, k_hbm, v_hbm,
                 wo_hbm, wg_hbm, wu_hbm, wd_hbm, x1_hbm, zt_ref, z_hbm, kn_ref, vn_ref,
                 pos_ref, cos_ref, sin_ref, gain1_ref, gain2_ref, x_ref, x1_ref, h2, q_ref, gain_row,
                 kbuf, vbuf, wo, o3, o2, ybuf, rb1, sb, rb2, tb, act, gbuf, wbuf,
                 small_sem, x_sem, q_sem, k_sem, v_sem, kc_sem, vc_sem, wo_sem, w_sem, x1_sem, z_sem,
                 s1, r1, s2, r2, s3, r3, s4, r4, s5, r5):
    tp = lax.axis_index("tp")
    mine = lax.rem(tp, 2)
    other = 1 - mine
    partner = tp + 1 - 2 * mine
    peer = lax.rem(tp + 2, 4)

    load_x = pltpu.make_async_copy(x_hbm, x_ref, x_sem)
    load_x.start()
    small = [pltpu.make_async_copy(src, dst, small_sem.at[i]) for i, (src, dst) in enumerate(
        ((gain1_hbm, gain1_ref), (gain2_hbm, gain2_ref), (cos_hbm, cos_ref), (sin_hbm, sin_ref), (pos_hbm, pos_ref)))]
    for copy in small:
        copy.start()

    def load_w(i):
        rows = pl.ds(i * KS, KS)
        kv = KVH * HD
        return (pltpu.make_async_copy(wq_hbm.at[rows, pl.ds(0, TN)], wbuf.at[0, rows], q_sem.at[0, i]),
                pltpu.make_async_copy(wq_hbm.at[rows, pl.ds(TN, TN)], wbuf.at[1, rows], q_sem.at[1, i]),
                pltpu.make_async_copy(wk_hbm.at[rows], wbuf.at[2, rows, pl.ds(0, kv)], k_sem.at[i]),
                pltpu.make_async_copy(wv_hbm.at[rows], wbuf.at[2, rows, pl.ds(kv, kv)], v_sem.at[i]))

    for i in range(2):
        for copy in load_w(i):
            copy.start()

    def load_kv(g):
        slot = lax.rem(g, KVSLOTS)
        seqs = pl.ds(g * BLK, BLK)
        return (pltpu.make_async_copy(k_hbm.at[seqs], kbuf.at[slot], kc_sem.at[slot]),
                pltpu.make_async_copy(v_hbm.at[seqs], vbuf.at[slot], vc_sem.at[slot]))

    load_wo = [pltpu.make_async_copy(wo_hbm.at[:, pl.ds(i * HALF, HALF)], wo.at[i], wo_sem.at[i]) for i in range(2)]

    barrier = pltpu.get_barrier_semaphore()
    for device in (partner, peer):
        pl.semaphore_signal(barrier, inc=1, device_id={"tp": device}, device_id_type=pl.DeviceIdType.MESH)

    for n in range(QKV // TN):
        ybuf[0, n] = jnp.zeros((SEQS, TN), F32)
    for copy in small:
        copy.wait()
    spread_gain(gain1_ref, gain_row)
    load_x.wait()
    for i in range(2, SLABS):
        for copy in load_w(i):
            copy.start()

    def norm_step(i, _):
        rows = pl.ds(pl.multiple_of(i * 16, 16), 16)
        total = jnp.zeros((16, 1), F32)
        for n in range(2 * NT):
            part = x_ref[rows, n * TN:(n + 1) * TN].astype(F32)
            total = total + jnp.sum(part * part, axis=1, keepdims=True)
        inv = lax.rsqrt(total * (1.0 / WIDTH) + EPS)
        for n in range(2 * NT):
            cols = slice(n * TN, (n + 1) * TN)
            h2[rows, cols] = (x_ref[rows, cols].astype(F32) * inv * gain_row[0:1, cols]).astype(BF16)
        return 0

    lax.fori_loop(0, SEQS // 16, norm_step, 0)

    def slab(i, _):
        for copy in load_w(i):
            copy.wait()
        rows = pl.ds(pl.multiple_of(i * KS, KS), KS)
        for n in range(QKV // TN):
            ybuf[0, n] += jnp.dot(h2[:, rows], wbuf[n, rows, :], preferred_element_type=F32)

        @pl.when(i < KVSLOTS)
        def _():
            for copy in load_kv(i):
                copy.start()

        @pl.when(i == KVSLOTS)
        def _():
            for copy in load_wo:
                copy.start()

        return 0

    lax.fori_loop(0, SLABS, slab, 0)

    def split(r, _):
        rows = pl.ds(pl.multiple_of(r * 32, 32), 32)
        cos_r = cos_ref[rows, :]
        sin_r = sin_ref[rows, :]

        def head(j):
            per = TN // HD
            return ybuf[0, j // per, rows, (j % per) * HD:(j % per + 1) * HD].astype(BF16).astype(F32)

        def rotate(v):
            return (v * cos_r + pltpu.roll(v, HD // 2, 1) * sin_r).astype(BF16).astype(F32)

        for j in range(QH):
            q_ref[pl.ds(pl.multiple_of(j * PITCH + r * 32, 8), 32), :] = rotate(head(j))
        for j in range(KVH):
            kn_ref[j, rows, :] = rotate(head(QH + j))
            vn_ref[j, rows, :] = head(QH + KVH + j)
        return 0

    lax.fori_loop(0, SEQS // 32, split, 0)
    spread_gain(gain2_ref, gain_row)
    pl.semaphore_wait(barrier, 2)

    def remote(src, dst, send, recv, device):
        return pltpu.make_async_remote_copy(src_ref=src, dst_ref=dst, send_sem=send, recv_sem=recv,
                                            device_id={"tp": device}, device_id_type=pl.DeviceIdType.MESH)

    def rows_of(c):
        return pl.ds(pl.multiple_of(c * ROWS, ROWS), ROWS)

    def send1(c):
        return remote(ybuf.at[other, :, rows_of(c)], rb1.at[:, rows_of(c)], s1.at[c], r1.at[c], partner)

    def send2(c):
        return remote(sb.at[:, rows_of(c)], rb2.at[:, rows_of(c)], s2.at[c], r2.at[c], peer)

    def send3(c):
        return remote(tb.at[mine, :, rows_of(c)], tb.at[mine, :, rows_of(c)], s3.at[c], r3.at[c], partner)

    def recv3(c):
        return remote(tb.at[other, :, rows_of(c)], tb.at[other, :, rows_of(c)], s3.at[c], r3.at[c], partner)

    def load_gate(t, slot):
        cols = pl.ds(pl.multiple_of(t * TN, TN), TN)
        return pltpu.make_async_copy(wg_hbm.at[:, cols], wbuf.at[slot], w_sem.at[slot])

    def load_up(t, slot):
        cols = pl.ds(pl.multiple_of(t * TN, TN), TN)
        return pltpu.make_async_copy(wu_hbm.at[:, cols], wbuf.at[slot], w_sem.at[slot])

    def load_down(t, slot):
        near = lax.rem(t, 2)
        half = near * mine + (1 - near) * other
        start = half * HALF + (t // 2) * TN
        cols = pl.ds(pl.multiple_of(start, TN), TN)
        return pltpu.make_async_copy(wd_hbm.at[:, cols], wbuf.at[slot, pl.ds(0, FFN)], w_sem.at[slot])

    def start_tile(i):
        slot = lax.rem(i, WSLOTS)
        odd = lax.rem(i, 2)

        @pl.when((i < 2 * GT) & (odd == 0))
        def _():
            load_gate(i // 2, slot).start()

        @pl.when((i < 2 * GT) & (odd == 1))
        def _():
            load_up(i // 2, slot).start()

        @pl.when((i >= 2 * GT) & (i < N_TILES))
        def _():
            load_down(i - 2 * GT, slot).start()

    col = lax.broadcasted_iota(jnp.int32, (QH, KVH * SLOTS), 1)
    row_head = lax.broadcasted_iota(jnp.int32, (QH, KVH * SLOTS), 0) // (QH // KVH)
    col_slot = jnp.where(lax.rem(col, KVH) == row_head, col // KVH, SLOTS)
    scale = 1.0 / math.sqrt(HD)
    low = lax.broadcasted_iota(jnp.int32, (QH, HD), 0) < QH // KVH

    def by_head(ref, b):
        return jnp.where(low, ref[0, pl.ds(b, 1), :], ref[1, pl.ds(b, 1), :])

    def attend(g, base):
        slot = lax.rem(g, KVSLOTS)
        for copy in load_kv(g):
            copy.wait()
        qs = [q_ref[pl.ds(g * BLK + i, QH, stride=PITCH), :] for i in range(BLK)]
        score = [lax.dot_general(qs[i].astype(BF16), kbuf[slot, i], (((1,), (1,)), ((), ())),
                                 preferred_element_type=F32) for i in range(BLK)]
        new = [jnp.sum(qs[i] * by_head(kn_ref, g * BLK + i), axis=1, keepdims=True) * scale for i in range(BLK)]
        score = [jnp.where(col_slot < pos_ref[g * BLK + i], score[i] * scale, -jnp.inf) for i in range(BLK)]
        top = [jnp.maximum(jnp.max(score[i], axis=1, keepdims=True), new[i]) for i in range(BLK)]
        e = [jnp.exp(score[i] - top[i]) for i in range(BLK)]
        e_new = [jnp.exp(new[i] - top[i]) for i in range(BLK)]
        inv = [1.0 / (jnp.sum(e[i], axis=1, keepdims=True) + e_new[i]) for i in range(BLK)]
        for i in range(BLK):
            prob = (e[i] * inv[i]).astype(BF16)
            prob_new = (e_new[i] * inv[i]).astype(BF16).astype(F32)
            out = jnp.dot(prob, vbuf[slot, i], preferred_element_type=F32)
            out = out + prob_new * by_head(vn_ref, g * BLK + i)
            o3[base + i] = out.astype(BF16).astype(F32)

        @pl.when(g + KVSLOTS < SEQS // BLK)
        def _():
            for copy in load_kv(g + KVSLOTS):
                copy.start()

    def project(c, half):
        for n in range(NT):
            ybuf[half, n, rows_of(c), :] = jnp.dot(o2[...], wo[half, :, n * TN:(n + 1) * TN],
                                                   preferred_element_type=F32)

    def stage2(c):
        send1(c).wait_recv()
        sb[:, rows_of(c)] = ybuf[mine, :, rows_of(c)] + rb1[:, rows_of(c)]
        send2(c).start()

    def stage3(c):
        send2(c).wait_recv()
        tb[mine, :, rows_of(c)] = sb[:, rows_of(c)] + rb2[:, rows_of(c)]
        send3(c).start()

    def stage4(c):
        recv3(c).wait_recv()

        def body(i, _):
            rows = pl.ds(pl.multiple_of(c * ROWS + i * 16, 16), 16)
            total = jnp.zeros((16, 1), F32)
            for half in range(2):
                for n in range(NT):
                    cols = slice(half * HALF + n * TN, half * HALF + (n + 1) * TN)
                    x1 = (x_ref[rows, cols].astype(F32) + tb[half, n, rows, :]).astype(BF16)
                    x1_ref[rows, cols] = x1
                    x1_f = x1.astype(F32)
                    total = total + jnp.sum(x1_f * x1_f, axis=1, keepdims=True)
            inv = lax.rsqrt(total * (1.0 / WIDTH) + EPS)
            for n in range(2 * NT):
                cols = slice(n * TN, (n + 1) * TN)
                h2[rows, cols] = (x1_ref[rows, cols].astype(F32) * inv * gain_row[0:1, cols]).astype(BF16)
            return 0

        lax.fori_loop(0, ROWS // 16, body, 0)

    def chunk(c, _):
        def block(j, _):
            attend(c * BLKS + j, j * BLK)

            @pl.when((j == 0) & (c >= 1))
            def _():
                stage2(c - 1)

            return 0

        lax.fori_loop(0, BLKS, block, 0)
        for j in range(QH):
            o2[:, j * HD:(j + 1) * HD] = o3[:, j, :].astype(BF16)

        @pl.when(c == 0)
        def _():
            for copy in load_wo:
                copy.wait()

        project(c, other)
        send1(c).start()
        project(c, mine)

        @pl.when(c >= CHUNKS - WSLOTS)
        def _():
            start_tile(c - (CHUNKS - WSLOTS))

        @pl.when(c >= 3)
        def _():
            stage3(c - 3)

        @pl.when(c >= 4)
        def _():
            stage4(c - 4)

        return 0

    lax.fori_loop(0, CHUNKS, chunk, 0)
    stage2(CHUNKS - 1)
    stage4(CHUNKS - 4)

    def gate_rows(t, rows):
        slot = lax.rem(2 * t, WSLOTS)
        for n in range(TN // 256):
            gbuf[rows, n * 256:(n + 1) * 256] = jnp.dot(h2[rows, :], wbuf[slot, :, n * 256:(n + 1) * 256],
                                                        preferred_element_type=F32).astype(BF16)

    def up_rows(t, rows):
        slot = lax.rem(2 * t + 1, WSLOTS)
        for n in range(TN // 256):
            up = jnp.dot(h2[rows, :], wbuf[slot, :, n * 256:(n + 1) * 256],
                         preferred_element_type=F32).astype(BF16).astype(F32)
            gate = gbuf[rows, n * 256:(n + 1) * 256].astype(F32)
            cols = pl.ds(pl.multiple_of(t * TN + n * 256, 256), 256)
            act[rows, cols] = (jax.nn.silu(gate) * up).astype(BF16)

    def gate_up_early(t, _):
        load_gate(t, lax.rem(2 * t, WSLOTS)).wait()
        gate_rows(t, slice(0, SEQS // 2))
        load_up(t, lax.rem(2 * t + 1, WSLOTS)).wait()
        up_rows(t, slice(0, SEQS // 2))
        return 0

    lax.fori_loop(0, EARLY, gate_up_early, 0)

    def tail(c, _):
        @pl.when(c < CHUNKS)
        def _():
            stage3(c)

        @pl.when(c > CHUNKS - 3)
        def _():
            stage4(c - 1)

        return 0

    lax.fori_loop(CHUNKS - 3, CHUNKS + 1, tail, 0)

    def sent(c, _):
        send1(c).wait_send()
        send2(c).wait_send()
        send3(c).wait_send()
        return 0

    lax.fori_loop(0, CHUNKS, sent, 0)

    save_x1 = pltpu.make_async_copy(x1_ref, x1_hbm, x1_sem)
    save_x1.start()

    def mm(lhs_ref, slot, depth, n):
        return jnp.dot(lhs_ref[...], wbuf[slot, 0:depth, n * 256:(n + 1) * 256], preferred_element_type=F32)

    def gate_up_late(t, _):
        gate_rows(t, slice(SEQS // 2, SEQS))
        start_tile(2 * t + WSLOTS)
        up_rows(t, slice(SEQS // 2, SEQS))
        start_tile(2 * t + 1 + WSLOTS)
        return 0

    lax.fori_loop(0, EARLY, gate_up_late, 0)

    def gate_up(t, _):
        load_gate(t, lax.rem(2 * t, WSLOTS)).wait()
        gate_rows(t, slice(0, SEQS))
        start_tile(2 * t + WSLOTS)
        load_up(t, lax.rem(2 * t + 1, WSLOTS)).wait()
        up_rows(t, slice(0, SEQS))
        start_tile(2 * t + 1 + WSLOTS)
        return 0

    lax.fori_loop(EARLY, GT, gate_up, 0)

    def send4(t):
        return remote(ybuf.at[other, t], rb1.at[t], s4.at[t], r4.at[t], partner)

    def save_z(t, j):
        return pltpu.make_async_copy(sb.at[t, pl.ds(j * PIECE, PIECE)], z_hbm.at[t * PER + j - 1], z_sem.at[t, j])

    send5 = remote(sb.at[0, pl.ds(0, PIECE)], rb2.at[0, pl.ds(0, PIECE)], s5, r5, peer)

    def down(t, _):
        i = 2 * GT + 2 * t
        slot = lax.rem(i, WSLOTS)
        load_down(2 * t, slot).wait()
        for n in range(TN // 256):
            ybuf[other, t, :, n * 256:(n + 1) * 256] = mm(act, slot, FFN, n)
        send4(t).start()
        start_tile(i + WSLOTS)
        slot = lax.rem(i + 1, WSLOTS)
        load_down(2 * t + 1, slot).wait()
        for n in range(TN // 256):
            sb[t, :, n * 256:(n + 1) * 256] = mm(act, slot, FFN, n)
        start_tile(i + 1 + WSLOTS)
        send4(t).wait_recv()
        sb[t] += rb1[t]

        @pl.when(t == 0)
        def _():
            send5.start()

        @pl.when(t > 0)
        def _():
            save_z(t, 0).start()

        for j in range(1, PER):
            save_z(t, j).start()
        return 0

    lax.fori_loop(0, NT, down, 0)

    def sent4(t, _):
        send4(t).wait_send()

        @pl.when(t > 0)
        def _():
            save_z(t, 0).wait()

        for j in range(1, PER):
            save_z(t, j).wait()
        return 0

    lax.fori_loop(0, NT, sent4, 0)
    save_x1.wait()
    send5.wait_send()
    send5.wait_recv()
    zt_ref[...] = sb[0, 0:PIECE] + rb2[0, 0:PIECE]


def layer(positions, cos_t, sin_t, gain1, gain2, resid_in, w_query, w_key, w_value, k_rows, v_rows, w_out,
          w_gate, w_up, w_down):
    vmem = pl.BlockSpec(memory_space=pltpu.VMEM)
    hbm = pl.BlockSpec(memory_space=pl.ANY)
    dma = pltpu.SemaphoreType.DMA
    shape = jax.ShapeDtypeStruct
    tile = (NT, SEQS, TN)
    return pl.pallas_call(
        layer_kernel,
        name="layer",
        out_shape=(shape((SEQS, WIDTH), BF16), shape((PIECE, TN), F32), shape((PIECES - 1, PIECE, TN), F32),
                   shape((KVH, SEQS, HD), F32), shape((KVH, SEQS, HD), F32)),
        in_specs=[hbm] * 15,
        out_specs=(hbm, vmem, hbm, vmem, vmem),
        scratch_shapes=[
            pltpu.SMEM((SEQS,), jnp.int32), pltpu.VMEM((SEQS, HD), F32), pltpu.VMEM((SEQS, HD), F32),
            pltpu.VMEM((32, 128), BF16), pltpu.VMEM((32, 128), BF16),
            pltpu.VMEM((SEQS, WIDTH), BF16), pltpu.VMEM((SEQS, WIDTH), BF16), pltpu.VMEM((SEQS, WIDTH), BF16),
            pltpu.VMEM((QH * PITCH, HD), F32), pltpu.VMEM((8, WIDTH), F32),
            pltpu.VMEM((KVSLOTS, BLK, KVH * SLOTS, HD), BF16), pltpu.VMEM((KVSLOTS, BLK, KVH * SLOTS, HD), BF16),
            pltpu.VMEM((2, QH * HD, HALF), BF16),
            pltpu.VMEM((ROWS, QH, HD), F32), pltpu.VMEM((ROWS, QH * HD), BF16),
            pltpu.VMEM((2,) + tile, F32), pltpu.VMEM(tile, F32), pltpu.VMEM(tile, F32),
            pltpu.VMEM(tile, F32), pltpu.VMEM((2,) + tile, F32),
            pltpu.VMEM((SEQS, FFN), BF16), pltpu.VMEM((SEQS, TN), BF16), pltpu.VMEM((WSLOTS, WIDTH, TN), BF16),
            dma((5,)), dma, dma((2, SLABS)), dma((SLABS,)), dma((SLABS,)), dma((KVSLOTS,)), dma((KVSLOTS,)),
            dma((2,)), dma((WSLOTS,)), dma, dma((NT, PER)),
            dma((CHUNKS,)), dma((CHUNKS,)), dma((CHUNKS,)), dma((CHUNKS,)), dma((CHUNKS,)), dma((CHUNKS,)),
            dma((NT,)), dma((NT,)), dma, dma],
        compiler_params=pltpu.CompilerParams(collective_id=0, has_side_effects=True, vmem_limit_bytes=VMEM_ALL),
        cost_estimate=pl.CostEstimate(flops=3 * 10**10, bytes_accessed=190 * 2**20, transcendentals=0),
    )(positions, cos_t, sin_t, gain1, gain2, resid_in, w_query, w_key, w_value, k_rows, v_rows, w_out,
      w_gate, w_up, w_down)


def final_kernel(zt_ref, z_ref, zr_ref, x1_ref, out_ref, tb, send_sem, recv_sem):
    tp = lax.axis_index("tp")
    mine = lax.rem(tp, 2)
    other = 1 - mine
    partner = tp + 1 - 2 * mine
    barrier = pltpu.get_barrier_semaphore()
    pl.semaphore_signal(barrier, inc=1, device_id={"tp": partner}, device_id_type=pl.DeviceIdType.MESH)
    pl.semaphore_wait(barrier, 1)

    def copy(half, t):
        return pltpu.make_async_remote_copy(src_ref=tb.at[half, t], dst_ref=tb.at[half, t], send_sem=send_sem.at[t],
                                            recv_sem=recv_sem.at[t], device_id={"tp": partner},
                                            device_id_type=pl.DeviceIdType.MESH)

    def add(half, t):
        cols = pl.ds(pl.multiple_of(half * HALF + t * TN, TN), TN)
        out_ref[:, cols] = (x1_ref[:, cols].astype(F32) + tb[half, t]).astype(BF16)

    for t in range(NT):
        for j in range(PER):
            p = t * PER + j - 1
            tb[mine, t, j * PIECE:(j + 1) * PIECE] = zt_ref[...] if p < 0 else z_ref[p] + zr_ref[p]
        copy(mine, t).start()
    for t in range(NT):
        add(mine, t)
    for t in range(NT):
        copy(other, t).wait_recv()
        add(other, t)
    for t in range(NT):
        copy(mine, t).wait_send()


def finish(z_first, z, z_peer, x1):
    vmem = pl.BlockSpec(memory_space=pltpu.VMEM)
    return pl.pallas_call(
        final_kernel,
        name="finish",
        out_shape=jax.ShapeDtypeStruct((SEQS, WIDTH), BF16),
        in_specs=[vmem] * 4,
        out_specs=vmem,
        scratch_shapes=[pltpu.VMEM((2, NT, SEQS, TN), F32), pltpu.SemaphoreType.DMA((NT,)),
                        pltpu.SemaphoreType.DMA((NT,))],
        compiler_params=pltpu.CompilerParams(collective_id=1, has_side_effects=True, vmem_limit_bytes=24 * 2**20),
        cost_estimate=pl.CostEstimate(flops=2 * 10**8, bytes_accessed=10 * 2**20, transcendentals=0),
    )(z_first, z, z_peer, x1)


def solution(mesh):
    def layer_local(resid_in, positions, k_cache, v_cache, gain_attn, w_query, w_key, w_value,
                    w_out, gain_mlp, w_gate, w_up, w_down):
        cos_t, sin_t = rope_tables(positions, HD)
        k_rows = k_cache.reshape(SEQS, SLOTS * KVH, HD)
        v_rows = v_cache.reshape(SEQS, SLOTS * KVH, HD)
        x1, z_first, z, kn, vn = layer(positions, cos_t, sin_t, gain_attn.reshape(32, 128), gain_mlp.reshape(32, 128),
                              resid_in, w_query, w_key, w_value, k_rows, v_rows, w_out, w_gate, w_up, w_down)
        z_peer = lax.ppermute(z, 'tp', [(0, 2), (1, 3), (2, 0), (3, 1)])
        k_full, v_full = write_caches(positions, kn, vn, k_cache, v_cache, z)
        resid_out = finish(z_first, z, z_peer, x1)
        return resid_out, k_full, v_full

    row_spec = P('dp', None)
    cache_spec = P('dp', None, 'tp', None)
    col_spec = P(None, 'tp')
    split_rows = P('tp', None)
    return jax.shard_map(layer_local, mesh=mesh,
                         in_specs=(row_spec, P('dp'), cache_spec, cache_spec, P(), col_spec, col_spec,
                                   col_spec, split_rows, P(), col_spec, col_spec, split_rows),
                         out_specs=(row_spec, cache_spec, cache_spec), check_vma=False)
```

```python
import functools
import math
import jax
import jax.numpy as jnp
import numpy as np
from jax import lax
from jax.experimental import pallas as pl
from jax.experimental.pallas import tpu as pltpu
from jax.sharding import PartitionSpec as P

EPS = 1e-5
ROPE_THETA = 500000.0
ROPE_FACTOR = 8.0
LOW_FACTOR = 1.0
HIGH_FACTOR = 4.0
ORIG_CTX = 8192.0

F32 = jnp.float32
BF16 = jnp.bfloat16
SEQS = 256
SLOTS = 256
WIDTH = 4096
HALF = WIDTH // 2
HD = 128
QH = 8
KVH = 2
FFN = 3584
VMEM_ALL = 67043328

ROWS = 32
CHUNKS = SEQS // ROWS
BLK = 8
BLKS = ROWS // BLK
KVSLOTS = 3
TN = 512
NT = HALF // TN
WSLOTS = 5
GT = FFN // TN
N_TILES = 2 * GT + 2 * NT
PIECE = 64
PIECES = NT * SEQS // PIECE
PER = SEQS // PIECE
EARLY = 2


def rope_tables(head_dim):
    half_dim = head_dim // 2
    lane = np.arange(head_dim)
    inv_freq = 1.0 / ROPE_THETA ** ((lane % half_dim) * (2.0 / head_dim))
    wavelen = (2.0 * math.pi) / inv_freq
    smooth = (ORIG_CTX / wavelen - LOW_FACTOR) / (HIGH_FACTOR - LOW_FACTOR)
    blended = (1.0 - smooth) * inv_freq / ROPE_FACTOR + smooth * inv_freq
    inv_freq = np.where(wavelen < ORIG_CTX / HIGH_FACTOR, inv_freq,
                        np.where(wavelen > ORIG_CTX / LOW_FACTOR, inv_freq / ROPE_FACTOR, blended))
    angles = np.arange(SLOTS, dtype=np.float32)[:, None] * inv_freq.astype(np.float32)[None, :]
    angles = angles.astype(np.float64)
    sign = np.where(lane < half_dim, -1.0, 1.0)
    shape = (SLOTS, 1, head_dim)
    return (np.cos(angles).astype(np.float32).reshape(shape), (np.sin(angles) * sign).astype(np.float32).reshape(shape))


CBLK = 8
CSLOTS = 24


def cache_kernel(pos_ref, kn_ref, vn_ref, k_hbm, v_hbm, after_hbm, k_out, v_out, buf, in_sem, out_sem):
    steps = [(src, dst, new, i) for i in range(SEQS // CBLK)
             for src, dst, new in ((k_hbm, k_out, kn_ref), (v_hbm, v_out, vn_ref))]
    n = len(steps)
    ahead = CSLOTS // 2

    def load(s):
        src, _, _, i = steps[s]
        return pltpu.make_async_copy(src.at[pl.ds(i * CBLK, CBLK)], buf.at[s % CSLOTS], in_sem.at[s % CSLOTS])

    def save(s):
        _, dst, _, i = steps[s]
        return pltpu.make_async_copy(buf.at[s % CSLOTS], dst.at[pl.ds(i * CBLK, CBLK)], out_sem.at[s % CSLOTS])

    for s in range(ahead):
        load(s).start()
    for s in range(n):
        if s + ahead < n:
            if s + ahead >= CSLOTS:
                save(s + ahead - CSLOTS).wait()
            load(s + ahead).start()
        load(s).wait()
        _, _, new, i = steps[s]

        def patch(j, _, new=new, i=i, s=s):
            row = i * CBLK + j
            pair = jnp.concatenate([new[h, pl.ds(row, 1), :] for h in range(KVH)], axis=0)
            buf[s % CSLOTS, j, pos_ref[row]] = pair.astype(BF16)
            return 0

        lax.fori_loop(0, CBLK, patch, 0)
        save(s).start()
    for s in range(n - CSLOTS, n):
        save(s).wait()


def write_caches(positions, kn, vn, k_cache, v_cache, after):
    vmem = pl.BlockSpec(memory_space=pltpu.VMEM)
    hbm = pl.BlockSpec(memory_space=pl.ANY)
    cache = jax.ShapeDtypeStruct(k_cache.shape, BF16)
    return pl.pallas_call(
        cache_kernel,
        name="write_caches",
        out_shape=(cache, cache),
        in_specs=[pl.BlockSpec(memory_space=pltpu.SMEM), vmem, vmem, hbm, hbm, hbm],
        out_specs=(hbm, hbm),
        scratch_shapes=[pltpu.VMEM((CSLOTS, CBLK, SLOTS, KVH, HD), BF16),
                        pltpu.SemaphoreType.DMA((CSLOTS,)), pltpu.SemaphoreType.DMA((CSLOTS,))],
        compiler_params=pltpu.CompilerParams(vmem_limit_bytes=56 * 2**20),
        cost_estimate=pl.CostEstimate(flops=2 * 10**10, bytes_accessed=128 * 2**20, transcendentals=0),
    )(positions, kn, vn, k_cache, v_cache, after)


KS = 512
SLABS = WIDTH // KS
PITCH = 264
QKV = (QH + 2 * KVH) * HD


def spread_gain(gain_ref, gain_row):
    for n in range(WIDTH // 128):
        gain_row[:, n * 128:(n + 1) * 128] = jnp.broadcast_to(gain_ref[n:n + 1, :].astype(F32), (8, 128))


def layer_kernel(pos_hbm, cos_hbm, sin_hbm, gain1_hbm, gain2_hbm, x_hbm, wq_hbm, wk_hbm, wv_hbm, k_hbm, v_hbm,
                 wo_hbm, wg_hbm, wu_hbm, wd_hbm, x1_hbm, zt_ref, z_hbm, kn_ref, vn_ref,
                 pos_ref, cos_tab, sin_tab, cos_ref, sin_ref, gain1_ref, gain2_ref, x_ref, x1_ref, h2, q_ref, gain_row,
                 kbuf, vbuf, wo, o3, o2, ybuf, rb1, sb, rb2, tb, act, gbuf, wbuf,
                 small_sem, x_sem, q_sem, k_sem, v_sem, kc_sem, vc_sem, wo_sem, w_sem, x1_sem, z_sem,
                 s1, r1, s2, r2, s3, r3, s4, r4, s5, r5):
    tp = lax.axis_index("tp")
    mine = lax.rem(tp, 2)
    other = 1 - mine
    partner = tp + 1 - 2 * mine
    peer = lax.rem(tp + 2, 4)

    load_x = pltpu.make_async_copy(x_hbm, x_ref, x_sem)
    load_x.start()
    small = [pltpu.make_async_copy(src, dst, small_sem.at[i]) for i, (src, dst) in enumerate(
        ((gain1_hbm, gain1_ref), (gain2_hbm, gain2_ref), (cos_hbm, cos_tab), (sin_hbm, sin_tab), (pos_hbm, pos_ref)))]
    for copy in small:
        copy.start()

    def load_w(i):
        rows = pl.ds(i * KS, KS)
        kv = KVH * HD
        return (pltpu.make_async_copy(wq_hbm.at[rows, pl.ds(0, TN)], wbuf.at[0, rows], q_sem.at[0, i]),
                pltpu.make_async_copy(wq_hbm.at[rows, pl.ds(TN, TN)], wbuf.at[1, rows], q_sem.at[1, i]),
                pltpu.make_async_copy(wk_hbm.at[rows], wbuf.at[2, rows, pl.ds(0, kv)], k_sem.at[i]),
                pltpu.make_async_copy(wv_hbm.at[rows], wbuf.at[2, rows, pl.ds(kv, kv)], v_sem.at[i]))

    for i in range(2):
        for copy in load_w(i):
            copy.start()

    def load_kv(g):
        slot = lax.rem(g, KVSLOTS)
        seqs = pl.ds(g * BLK, BLK)
        return (pltpu.make_async_copy(k_hbm.at[seqs], kbuf.at[slot], kc_sem.at[slot]),
                pltpu.make_async_copy(v_hbm.at[seqs], vbuf.at[slot], vc_sem.at[slot]))

    load_wo = [pltpu.make_async_copy(wo_hbm.at[:, pl.ds(i * HALF, HALF)], wo.at[i], wo_sem.at[i]) for i in range(2)]

    barrier = pltpu.get_barrier_semaphore()
    for device in (partner, peer):
        pl.semaphore_signal(barrier, inc=1, device_id={"tp": device}, device_id_type=pl.DeviceIdType.MESH)

    for n in range(QKV // TN):
        ybuf[0, n] = jnp.zeros((SEQS, TN), F32)
    for copy in small:
        copy.wait()
    spread_gain(gain1_ref, gain_row)

    def pick(i, _):
        for j in range(8):
            row = i * 8 + j
            pos = pos_ref[row]
            cos_ref[pl.ds(row, 1), :] = cos_tab[pos]
            sin_ref[pl.ds(row, 1), :] = sin_tab[pos]
        return 0

    lax.fori_loop(0, SEQS // 8, pick, 0)
    load_x.wait()
    for i in range(2, SLABS - 2):
        for copy in load_w(i):
            copy.start()

    def norm_step(i, _):
        rows = pl.ds(pl.multiple_of(i * 16, 16), 16)
        total = jnp.zeros((16, 1), F32)
        for n in range(2 * NT):
            part = x_ref[rows, n * TN:(n + 1) * TN].astype(F32)
            total = total + jnp.sum(part * part, axis=1, keepdims=True)
        inv = lax.rsqrt(total * (1.0 / WIDTH) + EPS)
        for n in range(2 * NT):
            cols = slice(n * TN, (n + 1) * TN)
            h2[rows, cols] = (x_ref[rows, cols].astype(F32) * inv * gain_row[0:1, cols]).astype(BF16)
        return 0

    lax.fori_loop(0, SEQS // 16, norm_step, 0)

    def slab(i, _):
        for copy in load_w(i):
            copy.wait()
        rows = pl.ds(pl.multiple_of(i * KS, KS), KS)
        for n in range(QKV // TN):
            ybuf[0, n] += jnp.dot(h2[:, rows], wbuf[n, rows, :], preferred_element_type=F32)

        @pl.when(i < 2)
        def _():
            for copy in load_w(i + SLABS - 2):
                copy.start()

        @pl.when(i < KVSLOTS)
        def _():
            for copy in load_kv(i):
                copy.start()

        @pl.when(i == KVSLOTS)
        def _():
            for copy in load_wo:
                copy.start()

        return 0

    lax.fori_loop(0, SLABS, slab, 0)

    def split(r, _):
        rows = pl.ds(pl.multiple_of(r * 32, 32), 32)
        cos_r = cos_ref[rows, :]
        sin_r = sin_ref[rows, :]

        def head(j):
            per = TN // HD
            return ybuf[0, j // per, rows, (j % per) * HD:(j % per + 1) * HD].astype(BF16).astype(F32)

        def rotate(v):
            return (v * cos_r + pltpu.roll(v, HD // 2, 1) * sin_r).astype(BF16).astype(F32)

        for j in range(QH):
            q_ref[pl.ds(pl.multiple_of(j * PITCH + r * 32, 8), 32), :] = rotate(head(j))
        for j in range(KVH):
            kn_ref[j, rows, :] = rotate(head(QH + j))
            vn_ref[j, rows, :] = head(QH + KVH + j)
        return 0

    lax.fori_loop(0, SEQS // 32, split, 0)
    spread_gain(gain2_ref, gain_row)
    pl.semaphore_wait(barrier, 2)

    def remote(src, dst, send, recv, device):
        return pltpu.make_async_remote_copy(src_ref=src, dst_ref=dst, send_sem=send, recv_sem=recv,
                                            device_id={"tp": device}, device_id_type=pl.DeviceIdType.MESH)

    def rows_of(c):
        return pl.ds(pl.multiple_of(c * ROWS, ROWS), ROWS)

    def send1(c):
        return remote(ybuf.at[other, :, rows_of(c)], rb1.at[:, rows_of(c)], s1.at[c], r1.at[c], partner)

    def send2(c):
        return remote(sb.at[:, rows_of(c)], rb2.at[:, rows_of(c)], s2.at[c], r2.at[c], peer)

    def send3(c):
        return remote(tb.at[mine, :, rows_of(c)], tb.at[mine, :, rows_of(c)], s3.at[c], r3.at[c], partner)

    def recv3(c):
        return remote(tb.at[other, :, rows_of(c)], tb.at[other, :, rows_of(c)], s3.at[c], r3.at[c], partner)

    def load_gate(t, slot):
        cols = pl.ds(pl.multiple_of(t * TN, TN), TN)
        return pltpu.make_async_copy(wg_hbm.at[:, cols], wbuf.at[slot], w_sem.at[slot])

    def load_up(t, slot):
        cols = pl.ds(pl.multiple_of(t * TN, TN), TN)
        return pltpu.make_async_copy(wu_hbm.at[:, cols], wbuf.at[slot], w_sem.at[slot])

    def load_down(t, slot):
        near = lax.rem(t, 2)
        half = near * mine + (1 - near) * other
        start = half * HALF + (t // 2) * TN
        cols = pl.ds(pl.multiple_of(start, TN), TN)
        return pltpu.make_async_copy(wd_hbm.at[:, cols], wbuf.at[slot, pl.ds(0, FFN)], w_sem.at[slot])

    def start_tile(i):
        slot = lax.rem(i, WSLOTS)
        odd = lax.rem(i, 2)

        @pl.when((i < 2 * GT) & (odd == 0))
        def _():
            load_gate(i // 2, slot).start()

        @pl.when((i < 2 * GT) & (odd == 1))
        def _():
            load_up(i // 2, slot).start()

        @pl.when((i >= 2 * GT) & (i < N_TILES))
        def _():
            load_down(i - 2 * GT, slot).start()

    col = lax.broadcasted_iota(jnp.int32, (QH, KVH * SLOTS), 1)
    row_head = lax.broadcasted_iota(jnp.int32, (QH, KVH * SLOTS), 0) // (QH // KVH)
    col_slot = jnp.where(lax.rem(col, KVH) == row_head, col // KVH, SLOTS)
    scale = 1.0 / math.sqrt(HD)
    low = lax.broadcasted_iota(jnp.int32, (QH, HD), 0) < QH // KVH

    def by_head(ref, b):
        return jnp.where(low, ref[0, pl.ds(b, 1), :], ref[1, pl.ds(b, 1), :])

    def attend(g, base):
        slot = lax.rem(g, KVSLOTS)
        for copy in load_kv(g):
            copy.wait()
        qs = [q_ref[pl.ds(g * BLK + i, QH, stride=PITCH), :] for i in range(BLK)]
        score = [lax.dot_general(qs[i].astype(BF16), kbuf[slot, i], (((1,), (1,)), ((), ())),
                                 preferred_element_type=F32) for i in range(BLK)]
        new = [jnp.sum(qs[i] * by_head(kn_ref, g * BLK + i), axis=1, keepdims=True) * scale for i in range(BLK)]
        score = [jnp.where(col_slot < pos_ref[g * BLK + i], score[i] * scale, -jnp.inf) for i in range(BLK)]
        top = [jnp.maximum(jnp.max(score[i], axis=1, keepdims=True), new[i]) for i in range(BLK)]
        e = [jnp.exp(score[i] - top[i]) for i in range(BLK)]
        e_new = [jnp.exp(new[i] - top[i]) for i in range(BLK)]
        inv = [1.0 / (jnp.sum(e[i], axis=1, keepdims=True) + e_new[i]) for i in range(BLK)]
        for i in range(BLK):
            prob = (e[i] * inv[i]).astype(BF16)
            prob_new = (e_new[i] * inv[i]).astype(BF16).astype(F32)
            out = jnp.dot(prob, vbuf[slot, i], preferred_element_type=F32)
            out = out + prob_new * by_head(vn_ref, g * BLK + i)
            o3[base + i] = out.astype(BF16).astype(F32)

        @pl.when(g + KVSLOTS < SEQS // BLK)
        def _():
            for copy in load_kv(g + KVSLOTS):
                copy.start()

    def project(c, half):
        for n in range(NT):
            ybuf[half, n, rows_of(c), :] = jnp.dot(o2[...], wo[half, :, n * TN:(n + 1) * TN],
                                                   preferred_element_type=F32)

    def stage2(c):
        send1(c).wait_recv()
        sb[:, rows_of(c)] = ybuf[mine, :, rows_of(c)] + rb1[:, rows_of(c)]
        send2(c).start()

    def stage3(c):
        send2(c).wait_recv()
        tb[mine, :, rows_of(c)] = sb[:, rows_of(c)] + rb2[:, rows_of(c)]
        send3(c).start()

    def stage4(c):
        recv3(c).wait_recv()

        def body(i, _):
            rows = pl.ds(pl.multiple_of(c * ROWS + i * 16, 16), 16)
            total = jnp.zeros((16, 1), F32)
            for half in range(2):
                for n in range(NT):
                    cols = slice(half * HALF + n * TN, half * HALF + (n + 1) * TN)
                    x1 = (x_ref[rows, cols].astype(F32) + tb[half, n, rows, :]).astype(BF16)
                    x1_ref[rows, cols] = x1
                    x1_f = x1.astype(F32)
                    total = total + jnp.sum(x1_f * x1_f, axis=1, keepdims=True)
            inv = lax.rsqrt(total * (1.0 / WIDTH) + EPS)
            for n in range(2 * NT):
                cols = slice(n * TN, (n + 1) * TN)
                h2[rows, cols] = (x1_ref[rows, cols].astype(F32) * inv * gain_row[0:1, cols]).astype(BF16)
            return 0

        lax.fori_loop(0, ROWS // 16, body, 0)

    def chunk(c, _):
        def block(j, _):
            attend(c * BLKS + j, j * BLK)

            @pl.when((j == 0) & (c >= 1))
            def _():
                stage2(c - 1)

            return 0

        lax.fori_loop(0, BLKS, block, 0)
        for j in range(QH):
            o2[:, j * HD:(j + 1) * HD] = o3[:, j, :].astype(BF16)

        @pl.when(c == 0)
        def _():
            for copy in load_wo:
                copy.wait()

        project(c, other)
        send1(c).start()
        project(c, mine)

        @pl.when(c >= CHUNKS - WSLOTS)
        def _():
            start_tile(c - (CHUNKS - WSLOTS))

        @pl.when(c >= 3)
        def _():
            stage3(c - 3)

        @pl.when(c >= 4)
        def _():
            stage4(c - 4)

        return 0

    lax.fori_loop(0, CHUNKS, chunk, 0)
    stage2(CHUNKS - 1)
    stage4(CHUNKS - 4)

    def gate_rows(t, rows):
        slot = lax.rem(2 * t, WSLOTS)
        for n in range(TN // 256):
            gbuf[rows, n * 256:(n + 1) * 256] = jnp.dot(h2[rows, :], wbuf[slot, :, n * 256:(n + 1) * 256],
                                                        preferred_element_type=F32).astype(BF16)

    def up_rows(t, rows):
        slot = lax.rem(2 * t + 1, WSLOTS)
        for n in range(TN // 256):
            up = jnp.dot(h2[rows, :], wbuf[slot, :, n * 256:(n + 1) * 256],
                         preferred_element_type=F32).astype(BF16).astype(F32)
            gate = gbuf[rows, n * 256:(n + 1) * 256].astype(F32)
            cols = pl.ds(pl.multiple_of(t * TN + n * 256, 256), 256)
            act[rows, cols] = (jax.nn.silu(gate) * up).astype(BF16)

    def gate_up_early(t, _):
        load_gate(t, lax.rem(2 * t, WSLOTS)).wait()
        gate_rows(t, slice(0, SEQS // 2))
        load_up(t, lax.rem(2 * t + 1, WSLOTS)).wait()
        up_rows(t, slice(0, SEQS // 2))
        return 0

    lax.fori_loop(0, EARLY, gate_up_early, 0)

    def tail(c, _):
        @pl.when(c < CHUNKS)
        def _():
            stage3(c)

        @pl.when(c > CHUNKS - 3)
        def _():
            stage4(c - 1)

        return 0

    lax.fori_loop(CHUNKS - 3, CHUNKS + 1, tail, 0)

    def sent(c, _):
        send1(c).wait_send()
        send2(c).wait_send()
        send3(c).wait_send()
        return 0

    lax.fori_loop(0, CHUNKS, sent, 0)

    save_x1 = pltpu.make_async_copy(x1_ref, x1_hbm, x1_sem)
    save_x1.start()

    def mm(lhs_ref, slot, depth, n):
        return jnp.dot(lhs_ref[...], wbuf[slot, 0:depth, n * 256:(n + 1) * 256], preferred_element_type=F32)

    def gate_up_late(t, _):
        gate_rows(t, slice(SEQS // 2, SEQS))
        start_tile(2 * t + WSLOTS)
        up_rows(t, slice(SEQS // 2, SEQS))
        start_tile(2 * t + 1 + WSLOTS)
        return 0

    lax.fori_loop(0, EARLY, gate_up_late, 0)

    def gate_up(t, _):
        load_gate(t, lax.rem(2 * t, WSLOTS)).wait()
        gate_rows(t, slice(0, SEQS))
        start_tile(2 * t + WSLOTS)
        load_up(t, lax.rem(2 * t + 1, WSLOTS)).wait()
        up_rows(t, slice(0, SEQS))
        start_tile(2 * t + 1 + WSLOTS)
        return 0

    lax.fori_loop(EARLY, GT, gate_up, 0)

    def send4(t):
        return remote(ybuf.at[other, t], rb1.at[t], s4.at[t], r4.at[t], partner)

    def save_z(t, j):
        return pltpu.make_async_copy(sb.at[t, pl.ds(j * PIECE, PIECE)], z_hbm.at[t * PER + j - 1], z_sem.at[t, j])

    send5 = remote(sb.at[0, pl.ds(0, PIECE)], rb2.at[0, pl.ds(0, PIECE)], s5, r5, peer)

    def down(t, _):
        i = 2 * GT + 2 * t
        slot = lax.rem(i, WSLOTS)
        load_down(2 * t, slot).wait()
        for n in range(TN // 256):
            ybuf[other, t, :, n * 256:(n + 1) * 256] = mm(act, slot, FFN, n)
        send4(t).start()
        start_tile(i + WSLOTS)
        slot = lax.rem(i + 1, WSLOTS)
        load_down(2 * t + 1, slot).wait()
        for n in range(TN // 256):
            sb[t, :, n * 256:(n + 1) * 256] = mm(act, slot, FFN, n)
        start_tile(i + 1 + WSLOTS)
        send4(t).wait_recv()
        sb[t] += rb1[t]

        @pl.when(t == 0)
        def _():
            send5.start()

        @pl.when(t > 0)
        def _():
            save_z(t, 0).start()

        for j in range(1, PER):
            save_z(t, j).start()
        return 0

    lax.fori_loop(0, NT, down, 0)

    def sent4(t, _):
        send4(t).wait_send()

        @pl.when(t > 0)
        def _():
            save_z(t, 0).wait()

        for j in range(1, PER):
            save_z(t, j).wait()
        return 0

    lax.fori_loop(0, NT, sent4, 0)
    save_x1.wait()
    send5.wait_send()
    send5.wait_recv()
    zt_ref[...] = sb[0, 0:PIECE] + rb2[0, 0:PIECE]


def layer(positions, cos_t, sin_t, gain1, gain2, resid_in, w_query, w_key, w_value, k_rows, v_rows, w_out,
          w_gate, w_up, w_down):
    vmem = pl.BlockSpec(memory_space=pltpu.VMEM)
    hbm = pl.BlockSpec(memory_space=pl.ANY)
    dma = pltpu.SemaphoreType.DMA
    shape = jax.ShapeDtypeStruct
    tile = (NT, SEQS, TN)
    return pl.pallas_call(
        layer_kernel,
        name="layer",
        out_shape=(shape((SEQS, WIDTH), BF16), shape((PIECE, TN), F32), shape((PIECES - 1, PIECE, TN), F32),
                   shape((KVH, SEQS, HD), F32), shape((KVH, SEQS, HD), F32)),
        in_specs=[hbm] * 15,
        out_specs=(hbm, vmem, hbm, vmem, vmem),
        scratch_shapes=[
            pltpu.SMEM((SEQS,), jnp.int32), pltpu.VMEM((SLOTS, 1, HD), F32), pltpu.VMEM((SLOTS, 1, HD), F32),
            pltpu.VMEM((SEQS, HD), F32), pltpu.VMEM((SEQS, HD), F32),
            pltpu.VMEM((32, 128), BF16), pltpu.VMEM((32, 128), BF16),
            pltpu.VMEM((SEQS, WIDTH), BF16), pltpu.VMEM((SEQS, WIDTH), BF16), pltpu.VMEM((SEQS, WIDTH), BF16),
            pltpu.VMEM((QH * PITCH, HD), F32), pltpu.VMEM((8, WIDTH), F32),
            pltpu.VMEM((KVSLOTS, BLK, KVH * SLOTS, HD), BF16), pltpu.VMEM((KVSLOTS, BLK, KVH * SLOTS, HD), BF16),
            pltpu.VMEM((2, QH * HD, HALF), BF16),
            pltpu.VMEM((ROWS, QH, HD), F32), pltpu.VMEM((ROWS, QH * HD), BF16),
            pltpu.VMEM((2,) + tile, F32), pltpu.VMEM(tile, F32), pltpu.VMEM(tile, F32),
            pltpu.VMEM(tile, F32), pltpu.VMEM((2,) + tile, F32),
            pltpu.VMEM((SEQS, FFN), BF16), pltpu.VMEM((SEQS, TN), BF16), pltpu.VMEM((WSLOTS, WIDTH, TN), BF16),
            dma((5,)), dma, dma((2, SLABS)), dma((SLABS,)), dma((SLABS,)), dma((KVSLOTS,)), dma((KVSLOTS,)),
            dma((2,)), dma((WSLOTS,)), dma, dma((NT, PER)),
            dma((CHUNKS,)), dma((CHUNKS,)), dma((CHUNKS,)), dma((CHUNKS,)), dma((CHUNKS,)), dma((CHUNKS,)),
            dma((NT,)), dma((NT,)), dma, dma],
        compiler_params=pltpu.CompilerParams(collective_id=0, has_side_effects=True, vmem_limit_bytes=VMEM_ALL),
        cost_estimate=pl.CostEstimate(flops=3 * 10**10, bytes_accessed=190 * 2**20, transcendentals=0),
    )(positions, cos_t, sin_t, gain1, gain2, resid_in, w_query, w_key, w_value, k_rows, v_rows, w_out,
      w_gate, w_up, w_down)


def final_kernel(zt_ref, z_ref, zr_ref, x1_ref, out_ref, tb, send_sem, recv_sem):
    tp = lax.axis_index("tp")
    mine = lax.rem(tp, 2)
    other = 1 - mine
    partner = tp + 1 - 2 * mine
    barrier = pltpu.get_barrier_semaphore()
    pl.semaphore_signal(barrier, inc=1, device_id={"tp": partner}, device_id_type=pl.DeviceIdType.MESH)
    pl.semaphore_wait(barrier, 1)

    def copy(half, t):
        return pltpu.make_async_remote_copy(src_ref=tb.at[half, t], dst_ref=tb.at[half, t], send_sem=send_sem.at[t],
                                            recv_sem=recv_sem.at[t], device_id={"tp": partner},
                                            device_id_type=pl.DeviceIdType.MESH)

    def add(half, t):
        cols = pl.ds(pl.multiple_of(half * HALF + t * TN, TN), TN)
        out_ref[:, cols] = (x1_ref[:, cols].astype(F32) + tb[half, t]).astype(BF16)

    for t in range(NT):
        for j in range(PER):
            p = t * PER + j - 1
            tb[mine, t, j * PIECE:(j + 1) * PIECE] = zt_ref[...] if p < 0 else z_ref[p] + zr_ref[p]
        copy(mine, t).start()
    for t in range(NT):
        add(mine, t)
    for t in range(NT):
        copy(other, t).wait_recv()
        add(other, t)
    for t in range(NT):
        copy(mine, t).wait_send()


def finish(z_first, z, z_peer, x1):
    vmem = pl.BlockSpec(memory_space=pltpu.VMEM)
    return pl.pallas_call(
        final_kernel,
        name="finish",
        out_shape=jax.ShapeDtypeStruct((SEQS, WIDTH), BF16),
        in_specs=[vmem] * 4,
        out_specs=vmem,
        scratch_shapes=[pltpu.VMEM((2, NT, SEQS, TN), F32), pltpu.SemaphoreType.DMA((NT,)),
                        pltpu.SemaphoreType.DMA((NT,))],
        compiler_params=pltpu.CompilerParams(collective_id=1, has_side_effects=True, vmem_limit_bytes=24 * 2**20),
        cost_estimate=pl.CostEstimate(flops=2 * 10**8, bytes_accessed=10 * 2**20, transcendentals=0),
    )(z_first, z, z_peer, x1)


def solution(mesh):
    def layer_local(resid_in, positions, k_cache, v_cache, gain_attn, w_query, w_key, w_value,
                    w_out, gain_mlp, w_gate, w_up, w_down):
        cos_t, sin_t = (jnp.asarray(table) for table in rope_tables(HD))
        k_rows = k_cache.reshape(SEQS, SLOTS * KVH, HD)
        v_rows = v_cache.reshape(SEQS, SLOTS * KVH, HD)
        x1, z_first, z, kn, vn = layer(positions, cos_t, sin_t, gain_attn.reshape(32, 128), gain_mlp.reshape(32, 128),
                              resid_in, w_query, w_key, w_value, k_rows, v_rows, w_out, w_gate, w_up, w_down)
        z_peer = lax.ppermute(z, 'tp', [(0, 2), (1, 3), (2, 0), (3, 1)])
        k_full, v_full = write_caches(positions, kn, vn, k_cache, v_cache, z)
        resid_out = finish(z_first, z, z_peer, x1)
        return resid_out, k_full, v_full

    row_spec = P('dp', None)
    cache_spec = P('dp', None, 'tp', None)
    col_spec = P(None, 'tp')
    split_rows = P('tp', None)
    return jax.shard_map(layer_local, mesh=mesh,
                         in_specs=(row_spec, P('dp'), cache_spec, cache_spec, P(), col_spec, col_spec,
                                   col_spec, split_rows, P(), col_spec, col_spec, split_rows),
                         out_specs=(row_spec, cache_spec, cache_spec), check_vma=False)
```
